128 devices in a mesh: dp: 64 (over z, y, x), mp: 2 (over core).
Axes of the slice: x: 4, y: 4, z: 4, core: 2. Of those that a mesh axis runs over, the one named last changes fastest.
Arguments:
- patches: bfloat16 [32768, 3200], P(('dp', 'mp')), may hold values from -120 to 120
- ln_gain: bfloat16 [3200], replicated, may hold values from 0.099609375 to 1.8984375
- ln_bias: bfloat16 [3200], replicated, may hold values from -3 to 3
- w_proj: bfloat16 [3200, 4096], P(None, 'mp'), may hold values from -0.109375 to 0.109375
- proj_bias: bfloat16 [4096], P('mp'), may hold values from -3 to 3
- rms_gain: bfloat16 [4096], replicated, may hold values from 0.099609375 to 1.8984375
- w_qkv: bfloat16 [4096, 3072], P(None, 'mp'), may hold values from -4 to 4
- image_counts: int32 [256, 8], replicated, may hold values from 1 to 16, as said below
- source_shift: int32 [32], replicated, may hold values from 0 to 63, as said below
Outputs:
- attended: bfloat16 [32768, 2048], P('dp', 'mp')
The draws below stay inside these ranges and needn't reach their ends.
Inputs may be any that keep to these rules, and one draw needn't show every extreme that they name: `image_counts`: row g holds the counts of the 8 images of tile g. In every draw all images of the tiles of some dp index hold 16 tokens. No value stands more than 1 times in source_shift, and some value stands exactly 1 times.
All inputs are finite; a program needn't handle non-finite values.
Results may differ from the reference program's by a relative error of at most 0.012.
Values may be sent and summed in bfloat16 or wider, within the bound.
No kernel may reach another device: no remote copies, remote signals or barrier semaphores. Data moves between devices by JAX's collectives and lax.ppermute only.
A program may use at most 128 MiB of HBM per device.

```python
import math
import jax
import jax.numpy as jnp
from jax import lax

D_VIT = 3200
MODEL_WIDTH = 4096
HEAD_SIZE = 128
TILE = 128
IMG_TILE = 8
TOK_DEV = 512
QUERY_PER_KEY = 4
TILES_DEV = 4
IMG_DEV = 32
IMG_MAX = 16
TOKENS = 32768
NTILES = 256
QKV_COLS = 3072
OUT_COLS = 2048
N_DP = 64


def draw_patches(key, part):
    base_key, row_key, col_key = jax.random.split(key, 3)
    row_scale = jnp.exp(jax.random.uniform(row_key, (TOKENS, 1), jnp.float32, 0.0, math.log(10.0)))
    col_scale = jnp.exp(jax.random.uniform(col_key, (1, D_VIT), jnp.float32, math.log(0.3), math.log(3.0)))
    base_values = jax.random.normal(base_key, (TOKENS, D_VIT), jnp.float32)
    return (jnp.clip(base_values, -4.0, 4.0) * row_scale * col_scale).astype(jnp.bfloat16)


def draw_w_qkv(key, part):
    base_key = jax.random.fold_in(key, 0)
    base_values = jnp.clip(jax.random.normal(base_key, (MODEL_WIDTH, QKV_COLS), jnp.float32), -5.0, 5.0) / math.sqrt(MODEL_WIDTH)
    return jnp.clip(base_values, -4.0, 4.0).astype(jnp.bfloat16)


def draw_image_counts(key, part):
    count_key, full_key = jax.random.split(key)
    counts = jax.random.randint(count_key, (NTILES, IMG_TILE), 1, IMG_MAX + 1, dtype=jnp.int32)
    full_device = jax.random.randint(full_key, (), 0, N_DP, dtype=jnp.int32)
    owner_dev = jnp.arange(NTILES, dtype=jnp.int32) // TILES_DEV
    return jnp.where((owner_dev == full_device)[:, None], IMG_MAX, counts).astype(jnp.int32)


def draw_source_shift(key, part):
    cycle_key, order_key = jax.random.split(key)
    random_rank = jax.random.permutation(cycle_key, N_DP).astype(jnp.int32)
    values_all = jnp.arange(N_DP, dtype=jnp.int32)
    scores = jnp.where(values_all == N_DP // 2, -3, jnp.where(values_all == N_DP - 1, -2, jnp.where(values_all == 1, -1, random_rank))).astype(jnp.int32)
    cycle_order = jnp.argsort(scores, stable=True).astype(jnp.int32)
    slot_order = jax.random.permutation(order_key, IMG_DEV).astype(jnp.int32)
    return cycle_order[slot_order % N_DP].astype(jnp.int32)


def shard_levels(stream_key, shape, shards, least, top_value):
    loudness = 1.0
    for axis_at, blocks in shards:
        heights = jax.random.uniform(jax.random.fold_in(jax.random.fold_in(stream_key, 6), axis_at), (blocks,), jnp.float32, least / len(shards), top_value / len(shards))
        loudness = loudness * jnp.repeat(jnp.exp(heights), shape[axis_at] // blocks).reshape((-1,) + (1,) * (len(shape) - 1 - axis_at))
    return loudness


def scatter_about(stream_key, dims, spread, most, cuts=(), kind=jnp.bfloat16):
    drawn = spread * jax.random.normal(stream_key, dims, jnp.float32)
    if cuts:
        drawn = drawn * shard_levels(stream_key, dims, cuts, -0.22, 0.18)
    return jnp.clip(drawn, -most, most).astype(kind)


def setup_inputs(seed: int = 0) -> dict:
    key_list = jax.random.split(jax.random.key(seed), 10)
    return {
        "patches": draw_patches(jax.random.fold_in(key_list[9], 71), 0),
        "ln_gain": jnp.clip(1.0 + 0.18 * jax.random.normal(key_list[1], (D_VIT,), jnp.float32), 0.099609375, 1.8984375).astype(jnp.bfloat16),
        "ln_bias": scatter_about(key_list[2], (D_VIT,), 0.5, 3.0),
        "w_proj": scatter_about(key_list[3], (D_VIT, MODEL_WIDTH), D_VIT ** -0.5, 0.109375, ((1, 2),)),
        "proj_bias": scatter_about(key_list[4], (MODEL_WIDTH,), 0.5, 3.0, ((0, 2),)),
        "rms_gain": jnp.clip(1.0 + 0.18 * jax.random.normal(key_list[5], (MODEL_WIDTH,), jnp.float32), 0.099609375, 1.8984375).astype(jnp.bfloat16),
        "w_qkv": draw_w_qkv(jax.random.fold_in(key_list[9], 71), 0),
        "image_counts": draw_image_counts(jax.random.fold_in(key_list[9], 71), 0),
        "source_shift": draw_source_shift(jax.random.fold_in(key_list[9], 71), 0),
    }


norm_epsilon = 1e-05
rms_epsilon = 1e-05
rotary_base = 500000.0

def routing(image_counts, source_shift):
    per_dest = image_counts.reshape(N_DP, IMG_DEV)
    senders = jnp.arange(N_DP, dtype=jnp.int32)
    dest_of = jnp.mod(senders[:, None] - source_shift[None, :], N_DP).astype(jnp.int32)
    sent_counts = jnp.take_along_axis(per_dest, dest_of, axis=0).astype(jnp.int32)
    starts = (jnp.cumsum(sent_counts, axis=1) - sent_counts).astype(jnp.int32)
    slot_ends = jnp.cumsum(image_counts, axis=1).astype(jnp.int32)
    offsets = (slot_ends - image_counts).astype(jnp.int32)
    position = jnp.arange(TILE, dtype=jnp.int32)
    slot_index = lax.optimization_barrier(jnp.sum((position[None, :, None] >= slot_ends[:, None, :]).astype(jnp.int32), axis=2)).astype(jnp.int32)
    live_rows = slot_index < IMG_TILE
    clipped = jnp.minimum(slot_index, IMG_TILE - 1).astype(jnp.int32)
    inside_tile = position[None, :] - jnp.take_along_axis(offsets, clipped, axis=1)
    tile_count = jnp.arange(NTILES, dtype=jnp.int32)
    owner_dev = tile_count // TILES_DEV
    image_k = ((tile_count % TILES_DEV)[:, None] * IMG_TILE + clipped).astype(jnp.int32)
    sender = jnp.mod(owner_dev[:, None] + source_shift[image_k], N_DP).astype(jnp.int32)
    source_row = sender * TOK_DEV + starts[sender, image_k] + inside_tile
    source_row = jnp.where(live_rows, source_row, 0).astype(jnp.int32)
    return (source_row.reshape(-1), live_rows.reshape(-1), slot_index.reshape(-1))

def layer_norm(row_block, gain_vec, bias_vec):
    values = row_block.astype(jnp.float32)
    row_mean = lax.optimization_barrier(jnp.mean(values, axis=-1, keepdims=True))
    centred = values - row_mean
    row_var = lax.optimization_barrier(jnp.mean(centred * centred, axis=-1, keepdims=True))
    scaled = centred * lax.rsqrt(row_var + norm_epsilon) * gain_vec.astype(jnp.float32)
    return (scaled + bias_vec.astype(jnp.float32)).astype(jnp.bfloat16)

def rotary(values, cos_table, sine_table):
    half_width = values.shape[-1] // 2
    turned = jnp.concatenate([-values[..., half_width:], values[..., :half_width]], axis=-1)
    return values * cos_table + turned * sine_table

def attend(queries, key_rows, value_rows, segment):
    tile_count = queries.shape[0] // TILE
    groups = queries.shape[1]
    query_f = queries.reshape(tile_count, TILE, groups, QUERY_PER_KEY, HEAD_SIZE).astype(jnp.float32)
    key_f = key_rows.reshape(tile_count, TILE, groups, HEAD_SIZE).astype(jnp.float32)
    value_f = value_rows.reshape(tile_count, TILE, groups, HEAD_SIZE).astype(jnp.float32)
    scores = jnp.einsum('tqhgd,tkhd->thgqk', query_f, key_f) * HEAD_SIZE ** (-0.5)
    segments = segment.reshape(tile_count, TILE)
    position = jnp.arange(TILE, dtype=jnp.int32)
    allowed = (position[None, :, None] >= position[None, None, :]) & (segments[:, :, None] == segments[:, None, :])
    scores = jnp.where(allowed[:, None, None], scores, -1e+30)
    row_max = lax.optimization_barrier(jnp.max(scores, axis=-1, keepdims=True))
    weights = jnp.exp(scores - row_max)
    probabilities = (weights / lax.optimization_barrier(jnp.sum(weights, axis=-1, keepdims=True))).astype(jnp.bfloat16)
    attended = jnp.einsum('thgqk,tkhd->tqhgd', probabilities.astype(jnp.float32), value_f)
    return attended.reshape(tile_count * TILE, groups * QUERY_PER_KEY * HEAD_SIZE)

def finish(hidden, live_flat, segment, rms_gain, w_qkv):
    row_total = hidden.shape[0]
    widened = hidden.astype(jnp.float32)
    mean_square = lax.optimization_barrier(jnp.mean(widened * widened, axis=-1, keepdims=True))
    rms_normed = (widened * lax.rsqrt(mean_square + rms_epsilon) * rms_gain.astype(jnp.float32)).astype(jnp.bfloat16)
    projections = jnp.dot(rms_normed, w_qkv, preferred_element_type=jnp.float32)
    groups = w_qkv.shape[1] // ((QUERY_PER_KEY + 2) * HEAD_SIZE)
    projections = projections.reshape(row_total, groups, QUERY_PER_KEY + 2, HEAD_SIZE)
    position = (jnp.arange(row_total, dtype=jnp.int32) % TILE).astype(jnp.float32)
    frequency = rotary_base ** (-(jnp.arange(HEAD_SIZE // 2, dtype=jnp.float32) * (2.0 / HEAD_SIZE)))
    angles = position[:, None] * frequency[None, :]
    cos_table = jnp.concatenate([jnp.cos(angles), jnp.cos(angles)], axis=-1)[:, None, None, :]
    sine_table = jnp.concatenate([jnp.sin(angles), jnp.sin(angles)], axis=-1)[:, None, None, :]
    queries = rotary(projections[:, :, :QUERY_PER_KEY], cos_table, sine_table).astype(jnp.bfloat16)
    key_rows = rotary(projections[:, :, QUERY_PER_KEY], cos_table[:, :, 0], sine_table[:, :, 0]).astype(jnp.bfloat16)
    value_rows = projections[:, :, QUERY_PER_KEY + 1].astype(jnp.bfloat16)
    attended = attend(queries, key_rows, value_rows, segment).astype(jnp.bfloat16)
    return jnp.where(live_flat[:, None], attended, jnp.zeros_like(attended))

def reference(patches, ln_gain, ln_bias, w_proj, proj_bias, rms_gain, w_qkv, image_counts, source_shift):
    source_row, live_rows, slot_index = routing(image_counts, source_shift)

    def device_block(device):
        pick_rows = lax.dynamic_slice_in_dim(source_row, device * TOK_DEV, TOK_DEV)
        live_flat = lax.dynamic_slice_in_dim(live_rows, device * TOK_DEV, TOK_DEV)
        segment = lax.dynamic_slice_in_dim(slot_index, device * TOK_DEV, TOK_DEV)
        gathered = jnp.take(patches, pick_rows, axis=0)
        normed = layer_norm(gathered, ln_gain, ln_bias)
        pre_act = jnp.dot(normed, w_proj, preferred_element_type=jnp.float32) + proj_bias.astype(jnp.float32)
        activated = jax.nn.gelu(pre_act, approximate=False)
        hidden = jnp.where(live_flat[:, None], activated, jnp.zeros_like(activated)).astype(jnp.bfloat16)
        return finish(hidden, live_flat, segment, rms_gain, w_qkv)
    blocks = lax.map(device_block, jnp.arange(N_DP, dtype=jnp.int32))
    return blocks.reshape(TOKENS, OUT_COLS)
```

```python
import functools

import jax
import jax.numpy as jnp
import numpy as np
from jax import lax
from jax.experimental import pallas as pl
from jax.experimental.pallas import tpu as pltpu
from jax.sharding import PartitionSpec as P

HEAD_SIZE = 128
TILE = 128
QUERY_PER_KEY = 4
IMG_MAX = 16

norm_epsilon = 1e-05
rms_epsilon = 1e-05
rotary_base = 500000.0

SWAP = [(0, 1), (1, 0)]
VMEM_BYTES = 56 * 1024 * 1024


def rotary_tables():
    half = HEAD_SIZE // 2
    frequency = rotary_base ** (-(np.arange(half, dtype=np.float64) * (2.0 / HEAD_SIZE)))
    angles = np.arange(IMG_MAX, dtype=np.float64)[:, None] * frequency[None, :]
    cos = np.concatenate([np.cos(angles), np.cos(angles)], axis=-1)
    sine = np.concatenate([-np.sin(angles), np.sin(angles)], axis=-1)
    return cos.astype(np.float32), sine.astype(np.float32)


def normalised(rows, gain, bias):
    values = rows.astype(jnp.float32)
    width = values.shape[-1]
    row_mean = jnp.sum(values, axis=-1, keepdims=True) * (1.0 / width)
    centred = values - row_mean
    row_var = jnp.sum(centred * centred, axis=-1, keepdims=True) * (1.0 / width)
    scaled = centred * lax.rsqrt(row_var + norm_epsilon) * gain.astype(jnp.float32)
    return (scaled + bias.astype(jnp.float32)).astype(jnp.bfloat16)


def norm_body(rows_ref, gain_ref, bias_ref, out_ref):
    out_ref[...] = normalised(rows_ref[...], gain_ref[...], bias_ref[...])


def layer_norm(rows, gain, bias):
    count, width = rows.shape
    step = 32
    return pl.pallas_call(
        norm_body,
        grid=(count // step,),
        in_specs=[
            pl.BlockSpec((step, width), lambda i: (i, 0)),
            pl.BlockSpec((1, width), lambda i: (0, 0)),
            pl.BlockSpec((1, width), lambda i: (0, 0)),
        ],
        out_specs=pl.BlockSpec((step, width), lambda i: (i, 0)),
        out_shape=jax.ShapeDtypeStruct((count, width), jnp.bfloat16),
        cost_estimate=pl.CostEstimate(
            flops=10 * count * width, bytes_accessed=4 * count * width, transcendentals=0
        ),
        name="layer_norm",
    )(rows, gain, bias)


def project_body(
    place_ref, counts_ref, shift_ref, own_ref, other_ref, gain_ref, bias_ref, w_ref, add_ref,
    out_ref, normed, align, acc,
):
    step = pl.program_id(0)
    last = pl.num_programs(0) - 1
    half = own_ref.shape[0]
    rows = 2 * half
    images = shift_ref.shape[0]
    senders = counts_ref.shape[0] // images

    @pl.when(step == 0)
    def _():
        core = place_ref[1]
        normed[pl.ds(pl.multiple_of(core * half, half), half), :] = own_ref[...]
        base = (1 - core) * half
        block = 32

        def fill(i, carry):
            src = pl.multiple_of(i * block, block)
            dst = pl.multiple_of(base + i * block, block)
            normed[pl.ds(dst, block), :] = normalised(
                other_ref[pl.ds(src, block), :], gain_ref[...], bias_ref[...]
            )
            return carry

        lax.fori_loop(0, half // block, fill, 0)
        column = lax.broadcasted_iota(jnp.int32, (IMG_MAX, rows), 1)
        inside = lax.broadcasted_iota(jnp.int32, (IMG_MAX, rows), 0)
        distance = column - inside
        start = jnp.int32(0)
        for k in range(images):
            align[k * IMG_MAX : (k + 1) * IMG_MAX, :] = jnp.where(
                distance == start, 1.0, 0.0
            ).astype(jnp.bfloat16)
            target = lax.rem(place_ref[0] - shift_ref[k] + senders, senders)
            start = start + counts_ref[target * images + k]

    def post():
        slot = lax.rem(step + 1, 2)
        pre = acc[slot] + add_ref[...].astype(jnp.float32)
        value = pre * (1.0 + lax.erf(pre * np.float32(0.5**0.5))) * 0.5
        out_ref[...] = jnp.dot(
            align[...], value.astype(jnp.bfloat16), preferred_element_type=jnp.float32
        ).astype(jnp.bfloat16)

    @pl.when(step < last)
    def _():
        acc[lax.rem(step, 2)] = jnp.dot(
            normed[...], w_ref[...], preferred_element_type=jnp.float32
        )
        post()

    @pl.when(step == last)
    def _():
        post()


def project(place, counts, shift, own, other, gain, bias, w_proj, proj_bias):
    half, width = own.shape
    rows = 2 * half
    columns = w_proj.shape[1]
    block = 256
    steps = columns // block
    whole = lambda j, *_: (0, 0)
    before = lambda j, *_: (0, jnp.maximum(j - 1, 0))
    return pl.pallas_call(
        project_body,
        grid_spec=pltpu.PrefetchScalarGridSpec(
            num_scalar_prefetch=3,
            grid=(steps + 1,),
            in_specs=[
                pl.BlockSpec((half, width), whole),
                pl.BlockSpec((half, width), whole),
                pl.BlockSpec((1, width), whole),
                pl.BlockSpec((1, width), whole),
                pl.BlockSpec((width, block), lambda j, *_: (0, jnp.minimum(j, steps - 1))),
                pl.BlockSpec((1, block), before),
            ],
            out_specs=pl.BlockSpec((rows, block), before),
            scratch_shapes=[
                pltpu.VMEM((rows, width), jnp.bfloat16),
                pltpu.VMEM((rows, rows), jnp.bfloat16),
                pltpu.VMEM((2, rows, block), jnp.float32),
            ],
        ),
        out_shape=jax.ShapeDtypeStruct((rows, columns), jnp.bfloat16),
        compiler_params=pltpu.CompilerParams(vmem_limit_bytes=VMEM_BYTES),
        cost_estimate=pl.CostEstimate(
            flops=2 * rows * width * columns,
            bytes_accessed=2 * width * columns,
            transcendentals=rows * columns,
        ),
        name="project",
    )(place, counts, shift, own, other, gain, bias, w_proj, proj_bias)


def lane_squares(values):
    total = None
    for c in range(values.shape[1] // 128):
        piece = values[:, c * 128 : (c + 1) * 128].astype(jnp.float32)
        total = piece * piece if total is None else total + piece * piece
    return total


def first_half_body(place_ref, hidden_ref, gain_ref, w_ref, part_ref, square_ref, gained):
    @pl.when(pl.program_id(0) == 0)
    def _():
        gained[...] = hidden_ref[...] * gain_ref[...]
        square_ref[...] = lane_squares(hidden_ref[...])

    part_ref[...] = jnp.dot(gained[...], w_ref[...], preferred_element_type=jnp.float32)


def first_half(place, hidden, rms_gain, w_qkv):
    rows, depth = hidden.shape
    columns = w_qkv.shape[1]
    block = 256
    return pl.pallas_call(
        first_half_body,
        grid_spec=pltpu.PrefetchScalarGridSpec(
            num_scalar_prefetch=1,
            grid=(columns // block,),
            in_specs=[
                pl.BlockSpec((rows, depth), lambda j, place: (0, 0)),
                pl.BlockSpec((1, depth), lambda j, place: (0, place[1])),
                pl.BlockSpec((depth, block), lambda j, place: (place[1], j)),
            ],
            out_specs=[
                pl.BlockSpec((rows, block), lambda j, place: (0, j)),
                pl.BlockSpec((rows, 128), lambda j, place: (0, 0)),
            ],
            scratch_shapes=[pltpu.VMEM((rows, depth), jnp.bfloat16)],
        ),
        out_shape=[
            jax.ShapeDtypeStruct((rows, columns), jnp.float32),
            jax.ShapeDtypeStruct((rows, 128), jnp.float32),
        ],
        compiler_params=pltpu.CompilerParams(vmem_limit_bytes=VMEM_BYTES),
        cost_estimate=pl.CostEstimate(
            flops=2 * rows * depth * columns,
            bytes_accessed=2 * depth * columns + 4 * rows * columns,
            transcendentals=0,
        ),
        name="first_half",
    )(place, hidden, rms_gain, w_qkv)


def attend_body(
    place_ref, shift_ref, hidden_ref, gain_ref, w_ref, part_ref, square_ref, cos_ref, sine_ref,
    out_ref, gained, factor, heads,
):
    step = pl.program_id(0)
    rows, depth = hidden_ref.shape
    images = shift_ref.shape[0]
    senders = out_ref.shape[0]
    per_tile = TILE // IMG_MAX

    @pl.when(step == 0)
    def _():
        gained[...] = hidden_ref[...] * gain_ref[...]
        squares = square_ref[...] + lane_squares(hidden_ref[...])
        mean_square = jnp.sum(squares, axis=-1, keepdims=True) * (1.0 / (2 * depth))
        factor[...] = jnp.broadcast_to(lax.rsqrt(mean_square + rms_epsilon), factor.shape)

    def product():
        heads[lax.rem(step, 2)] = part_ref[...] + jnp.dot(
            gained[...], w_ref[...], preferred_element_type=jnp.float32
        )

    def rotated(values):
        values = values.reshape(per_tile, IMG_MAX, HEAD_SIZE)
        turned = pltpu.roll(values, HEAD_SIZE // 2, 2)
        mixed = values * cos_ref[...][None] + turned * sine_ref[...][None]
        return mixed.reshape(TILE, HEAD_SIZE).astype(jnp.bfloat16)

    def attention(group):
        slot = group % 2
        q_at = lax.broadcasted_iota(jnp.int32, (QUERY_PER_KEY * TILE, TILE), 0)
        k_at = lax.broadcasted_iota(jnp.int32, (QUERY_PER_KEY * TILE, TILE), 1)
        q_at = jnp.bitwise_and(q_at, TILE - 1)
        allowed = (q_at >= k_at) & ((q_at // IMG_MAX) == (k_at // IMG_MAX))
        for tile in range(rows // TILE):
            at = slice(tile * TILE, (tile + 1) * TILE)
            scale = factor[at, :]

            def head(n):
                return heads[slot, at, n * HEAD_SIZE : (n + 1) * HEAD_SIZE] * scale

            queries = jnp.concatenate([rotated(head(n)) for n in range(QUERY_PER_KEY)], axis=0)
            key_rows = rotated(head(QUERY_PER_KEY))
            value_rows = head(QUERY_PER_KEY + 1).astype(jnp.bfloat16)
            scores = lax.dot_general(
                queries, key_rows, (((1,), (1,)), ((), ())), preferred_element_type=jnp.float32
            ) * np.float32(HEAD_SIZE**-0.5)
            scores = jnp.where(allowed, scores, -1e30)
            weights = jnp.exp(scores - jnp.max(scores, axis=-1, keepdims=True))
            inverse = 1.0 / jnp.sum(weights, axis=-1, keepdims=True)
            probabilities = (weights * inverse).astype(jnp.bfloat16)
            attended = jnp.dot(
                probabilities, value_rows, preferred_element_type=jnp.float32
            ).astype(jnp.bfloat16)
            for j in range(per_tile):
                k = tile * per_tile + j
                target = lax.rem(place_ref[0] - shift_ref[k] + senders, senders)
                for n in range(QUERY_PER_KEY):
                    column = (group * QUERY_PER_KEY + n) * HEAD_SIZE
                    out_ref[target, :, column : column + HEAD_SIZE] = attended[
                        n * TILE + j * IMG_MAX : n * TILE + (j + 1) * IMG_MAX, :
                    ]

    groups = pl.num_programs(0) - 1
    del groups

    @pl.when(step == 0)
    def _():
        product()

    @pl.when(step == 1)
    def _():
        product()
        attention(0)

    @pl.when(step == 2)
    def _():
        attention(1)


def attend(place, shift, hidden, rms_gain, w_qkv, part, square, senders):
    rows, depth = hidden.shape
    block = (QUERY_PER_KEY + 2) * HEAD_SIZE
    groups = w_qkv.shape[1] // block
    out_columns = groups * QUERY_PER_KEY * HEAD_SIZE
    cos, sine = rotary_tables()
    whole = lambda j, *_: (0, 0)
    return pl.pallas_call(
        attend_body,
        grid_spec=pltpu.PrefetchScalarGridSpec(
            num_scalar_prefetch=2,
            grid=(groups + 1,),
            in_specs=[
                pl.BlockSpec((rows, depth), whole),
                pl.BlockSpec((1, depth), lambda j, place, shift: (0, 1 - place[1])),
                pl.BlockSpec(
                    (depth, block),
                    lambda j, place, shift: (1 - place[1], jnp.minimum(j, groups - 1)),
                ),
                pl.BlockSpec((rows, block), lambda j, *_: (0, jnp.minimum(j, groups - 1))),
                pl.BlockSpec((rows, 128), whole),
                pl.BlockSpec((IMG_MAX, HEAD_SIZE), whole),
                pl.BlockSpec((IMG_MAX, HEAD_SIZE), whole),
            ],
            out_specs=pl.BlockSpec((senders, IMG_MAX, out_columns), lambda j, *_: (0, 0, 0)),
            scratch_shapes=[
                pltpu.VMEM((rows, depth), jnp.bfloat16),
                pltpu.VMEM((rows, HEAD_SIZE), jnp.float32),
                pltpu.VMEM((2, rows, block), jnp.float32),
            ],
        ),
        out_shape=jax.ShapeDtypeStruct((senders, IMG_MAX, out_columns), jnp.bfloat16),
        compiler_params=pltpu.CompilerParams(vmem_limit_bytes=VMEM_BYTES),
        cost_estimate=pl.CostEstimate(
            flops=2 * rows * depth * groups * block,
            bytes_accessed=2 * depth * groups * block,
            transcendentals=0,
        ),
        name="attend",
    )(place, shift, hidden, rms_gain, w_qkv, part, square, jnp.asarray(cos), jnp.asarray(sine))


def place_body(place_ref, counts_ref, shift_ref, box_ref, out_ref):
    tile = pl.program_id(0)
    senders = box_ref.shape[0]
    images = shift_ref.shape[0]
    per_tile = TILE // IMG_MAX
    lane = lax.broadcasted_iota(jnp.int32, (TILE, TILE), 1)
    row = lax.broadcasted_iota(jnp.int32, (TILE, TILE), 0)
    inside = jnp.bitwise_and(lane, IMG_MAX - 1)
    image = lane // IMG_MAX
    pick = jnp.zeros((TILE, TILE), jnp.bool_)
    offset = jnp.int32(0)
    blocks = []
    for j in range(per_tile):
        k = tile * per_tile + j
        count = counts_ref[place_ref[0] * images + k]
        hit = (image == j) & (row == inside + offset) & (inside < count)
        pick = pick | hit
        offset = offset + count
        source = lax.rem(place_ref[0] + shift_ref[k], senders)
        blocks.append(box_ref[source])
    out_ref[...] = jnp.dot(
        jnp.where(pick, 1.0, 0.0).astype(jnp.bfloat16),
        jnp.concatenate(blocks, axis=0),
        preferred_element_type=jnp.float32,
    ).astype(jnp.bfloat16)


def place_rows(place, counts, shift, box):
    senders, depth, columns = box.shape
    tiles = shift.shape[0] * depth // TILE
    return pl.pallas_call(
        place_body,
        grid_spec=pltpu.PrefetchScalarGridSpec(
            num_scalar_prefetch=3,
            grid=(tiles,),
            in_specs=[pl.BlockSpec((senders, depth, columns), lambda i, *_: (0, 0, 0))],
            out_specs=pl.BlockSpec((TILE, columns), lambda i, *_: (i, 0)),
        ),
        out_shape=jax.ShapeDtypeStruct((tiles * TILE, columns), jnp.bfloat16),
        compiler_params=pltpu.CompilerParams(vmem_limit_bytes=VMEM_BYTES),
        name="place_rows",
    )(place, counts, shift, box)


def local(
    patches, ln_gain, ln_bias, w_proj, proj_bias, rms_gain, w_qkv, image_counts, source_shift
):
    senders = lax.axis_size("dp")
    place = jnp.stack([lax.axis_index("dp"), lax.axis_index("mp")]).astype(jnp.int32)
    counts = image_counts.reshape(-1)
    other = lax.ppermute(patches, "mp", SWAP)
    gain = ln_gain.reshape(1, -1)
    bias = ln_bias.reshape(1, -1)
    own = layer_norm(patches, gain, bias)
    hidden = project(
        place, counts, source_shift, own, other, gain, bias, w_proj, proj_bias.reshape(1, -1)
    )
    far_hidden = lax.ppermute(hidden, "mp", SWAP)
    rms_row = rms_gain.reshape(1, -1)
    part, square = first_half(place, hidden, rms_row, w_qkv)
    outbox = attend(place, source_shift, far_hidden, rms_row, w_qkv, part, square, senders)
    in_box = lax.all_to_all(outbox, "dp", split_axis=0, concat_axis=0, tiled=True)
    return place_rows(place, counts, source_shift, in_box)


def solution(mesh):
    in_specs = (
        P(("dp", "mp"), None),
        P(),
        P(),
        P(None, "mp"),
        P("mp"),
        P(),
        P(None, "mp"),
        P(),
        P(),
    )
    out_specs = P("dp", "mp")
    return jax.shard_map(local, mesh=mesh, in_specs=in_specs, out_specs=out_specs, check_vma=False)
```

```python
import functools

import jax
import jax.numpy as jnp
import numpy as np
from jax import lax
from jax.experimental import pallas as pl
from jax.experimental.pallas import tpu as pltpu
from jax.sharding import PartitionSpec as P

HEAD_SIZE = 128
TILE = 128
QUERY_PER_KEY = 4
IMG_MAX = 16

norm_epsilon = 1e-05
rms_epsilon = 1e-05
rotary_base = 500000.0

SWAP = [(0, 1), (1, 0)]


def rotary_tables():
    half = HEAD_SIZE // 2
    frequency = rotary_base ** (-(np.arange(half, dtype=np.float64) * (2.0 / HEAD_SIZE)))
    angles = np.arange(IMG_MAX, dtype=np.float64)[:, None] * frequency[None, :]
    cos = np.concatenate([np.cos(angles), np.cos(angles)], axis=-1)
    sine = np.concatenate([-np.sin(angles), np.sin(angles)], axis=-1)
    return cos.astype(np.float32), sine.astype(np.float32)


def normalised(rows, gain, bias):
    values = rows.astype(jnp.float32)
    width = values.shape[-1]
    row_mean = jnp.sum(values, axis=-1, keepdims=True) * (1.0 / width)
    centred = values - row_mean
    row_var = jnp.sum(centred * centred, axis=-1, keepdims=True) * (1.0 / width)
    scaled = centred * lax.rsqrt(row_var + norm_epsilon) * gain.astype(jnp.float32)
    return (scaled + bias.astype(jnp.float32)).astype(jnp.bfloat16)


WHOLE = pl.BlockSpec(memory_space=pltpu.VMEM)
SCALARS = pl.BlockSpec(memory_space=pltpu.SMEM)
NORM_ROWS = 32
COLUMNS = 256


def limit(mib):
    return pltpu.CompilerParams(vmem_limit_bytes=mib * 1024 * 1024)


def fill_normed(src_ref, gain_ref, bias_ref, dst_ref, base):
    width = src_ref.shape[1]
    gain = gain_ref[...].reshape(1, width)
    bias = bias_ref[...].reshape(1, width)

    def fill(i, carry):
        src = pl.multiple_of(i * NORM_ROWS, NORM_ROWS)
        dst = pl.multiple_of(base + i * NORM_ROWS, NORM_ROWS)
        dst_ref[pl.ds(dst, NORM_ROWS), :] = normalised(
            src_ref[pl.ds(src, NORM_ROWS), :], gain, bias
        )
        return carry

    lax.fori_loop(0, src_ref.shape[0] // NORM_ROWS, fill, 0)


def norm_body(rows_ref, gain_ref, bias_ref, out_ref):
    fill_normed(rows_ref, gain_ref, bias_ref, out_ref, 0)


def layer_norm(rows, gain, bias):
    count, width = rows.shape
    return pl.pallas_call(
        norm_body,
        in_specs=[WHOLE] * 3,
        out_specs=WHOLE,
        out_shape=jax.ShapeDtypeStruct((count, width), jnp.bfloat16),
        compiler_params=limit(8),
        cost_estimate=pl.CostEstimate(
            flops=6_000_000_000, bytes_accessed=4 * count * width, transcendentals=0
        ),
        name="layer_norm",
    )(rows, gain, bias)


def project_body(
    counts_ref, shift_ref, own_ref, other_ref, gain_ref, bias_ref, w_ref, add_ref,
    out_ref, normed, align, acc_even, acc_odd,
):
    half = own_ref.shape[0]
    rows = 2 * half
    images = shift_ref.shape[0]
    tile_images = counts_ref.shape[0]
    tiles = images // tile_images
    senders = counts_ref.shape[1] // tiles
    blocks = w_ref.shape[1] // COLUMNS
    core = lax.axis_index("mp")
    me = lax.axis_index("dp")

    normed[pl.ds(pl.multiple_of(core * half, half), half), :] = own_ref[...]
    fill_normed(other_ref, gain_ref, bias_ref, normed, (1 - core) * half)
    column = lax.broadcasted_iota(jnp.int32, (IMG_MAX, rows), 1)
    inside = lax.broadcasted_iota(jnp.int32, (IMG_MAX, rows), 0)
    distance = column - inside
    start = jnp.int32(0)
    for k in range(images):
        align[k * IMG_MAX : (k + 1) * IMG_MAX, :] = jnp.where(distance == start, 1.0, 0.0).astype(
            jnp.bfloat16
        )
        target = lax.rem(me - shift_ref[k] + senders, senders)
        start = start + counts_ref[k % tile_images, target * tiles + k // tile_images]

    def product(block, acc):
        at = pl.multiple_of(block * COLUMNS, COLUMNS)
        acc[...] = jnp.dot(
            normed[...], w_ref[:, pl.ds(at, COLUMNS)], preferred_element_type=jnp.float32
        )

    def post(block, acc):
        at = pl.multiple_of(block * COLUMNS, COLUMNS)
        pre = acc[...] + add_ref[:, pl.ds(at, COLUMNS)].astype(jnp.float32)
        value = pre * (1.0 + lax.erf(pre * np.float32(0.5**0.5))) * 0.5
        out_ref[:, pl.ds(at, COLUMNS)] = jnp.dot(
            align[...], value.astype(jnp.bfloat16), preferred_element_type=jnp.float32
        ).astype(jnp.bfloat16)

    acc_odd[...] = jnp.zeros_like(acc_odd)

    def pair(p, carry):
        product(2 * p, acc_even)
        post(jnp.maximum(2 * p - 1, 0), acc_odd)
        product(2 * p + 1, acc_odd)
        post(2 * p, acc_even)
        return carry

    lax.fori_loop(0, blocks // 2, pair, 0)
    post(blocks - 1, acc_odd)


def project(counts, shift, own, other, gain, bias, w_proj, proj_bias):
    half, width = own.shape
    rows = 2 * half
    columns = w_proj.shape[1]
    return pl.pallas_call(
        project_body,
        in_specs=[SCALARS] * 2 + [WHOLE] * 6,
        out_specs=WHOLE,
        scratch_shapes=[
            pltpu.VMEM((rows, width), jnp.bfloat16),
            pltpu.VMEM((rows, rows), jnp.bfloat16),
            pltpu.VMEM((rows, COLUMNS), jnp.float32),
            pltpu.VMEM((rows, COLUMNS), jnp.float32),
        ],
        out_shape=jax.ShapeDtypeStruct((rows, columns), jnp.bfloat16),
        compiler_params=limit(12),
        cost_estimate=pl.CostEstimate(
            flops=2 * rows * width * columns,
            bytes_accessed=2 * width * columns,
            transcendentals=rows * columns,
        ),
        name="project",
    )(counts, shift, own, other, gain, bias, w_proj, proj_bias)


def lane_squares(values):
    total = None
    for c in range(values.shape[1] // 128):
        piece = values[:, c * 128 : (c + 1) * 128].astype(jnp.float32)
        total = piece * piece if total is None else total + piece * piece
    return total


def first_half_body(hidden_ref, gain_ref, w_ref, part_ref, square_ref, gained):
    depth = hidden_ref.shape[1]
    mine = pl.multiple_of(lax.axis_index("mp") * depth, depth)
    gained[...] = hidden_ref[...] * gain_ref[:, pl.ds(mine, depth)]
    square_ref[...] = lane_squares(hidden_ref[...])

    def block(j, carry):
        at = pl.multiple_of(j * COLUMNS, COLUMNS)
        part_ref[:, pl.ds(at, COLUMNS)] = jnp.dot(
            gained[...], w_ref[pl.ds(mine, depth), pl.ds(at, COLUMNS)],
            preferred_element_type=jnp.float32,
        )
        return carry

    lax.fori_loop(0, w_ref.shape[1] // COLUMNS, block, 0)


def first_half(hidden, rms_gain, w_qkv):
    rows, depth = hidden.shape
    columns = w_qkv.shape[1]
    return pl.pallas_call(
        first_half_body,
        in_specs=[WHOLE] * 3,
        out_specs=[WHOLE] * 2,
        scratch_shapes=[pltpu.VMEM((rows, depth), jnp.bfloat16)],
        out_shape=[
            jax.ShapeDtypeStruct((rows, columns), jnp.float32),
            jax.ShapeDtypeStruct((rows, 128), jnp.float32),
        ],
        compiler_params=limit(8),
        cost_estimate=pl.CostEstimate(
            flops=2 * rows * depth * columns,
            bytes_accessed=2 * depth * columns + 4 * rows * columns,
            transcendentals=0,
        ),
        name="first_half",
    )(hidden, rms_gain, w_qkv)


def attend_body(
    shift_ref, hidden_ref, gain_ref, w_ref, part_ref, square_ref, cos_ref, sine_ref,
    out_ref, gained, factor, *heads,
):
    rows, depth = hidden_ref.shape
    senders = out_ref.shape[0]
    per_tile = TILE // IMG_MAX
    width = heads[0].shape[1]
    me = lax.axis_index("dp")
    far = pl.multiple_of((1 - lax.axis_index("mp")) * depth, depth)

    gained[...] = hidden_ref[...] * gain_ref[:, pl.ds(far, depth)]
    squares = square_ref[...] + lane_squares(hidden_ref[...])
    mean_square = jnp.sum(squares, axis=-1, keepdims=True) * (1.0 / (2 * depth))
    factor[...] = jnp.broadcast_to(lax.rsqrt(mean_square + rms_epsilon), factor.shape)

    def product(group):
        at = slice(group * width, (group + 1) * width)
        heads[group][...] = part_ref[:, at] + jnp.dot(
            gained[...], w_ref[pl.ds(far, depth), at], preferred_element_type=jnp.float32
        )

    def rotated(values):
        values = values.reshape(per_tile, IMG_MAX, HEAD_SIZE)
        turned = pltpu.roll(values, HEAD_SIZE // 2, 2)
        mixed = values * cos_ref[...][None] + turned * sine_ref[...][None]
        return mixed.reshape(TILE, HEAD_SIZE).astype(jnp.bfloat16)

    q_at = lax.broadcasted_iota(jnp.int32, (QUERY_PER_KEY * TILE, TILE), 0)
    k_at = lax.broadcasted_iota(jnp.int32, (QUERY_PER_KEY * TILE, TILE), 1)
    q_at = jnp.bitwise_and(q_at, TILE - 1)
    allowed = (q_at >= k_at) & ((q_at // IMG_MAX) == (k_at // IMG_MAX))

    def attention(group):
        for tile in range(rows // TILE):
            at = slice(tile * TILE, (tile + 1) * TILE)
            scale = factor[at, :]

            def head(n):
                return heads[group][at, n * HEAD_SIZE : (n + 1) * HEAD_SIZE] * scale

            queries = jnp.concatenate([rotated(head(n)) for n in range(QUERY_PER_KEY)], axis=0)
            key_rows = rotated(head(QUERY_PER_KEY))
            value_rows = head(QUERY_PER_KEY + 1).astype(jnp.bfloat16)
            scores = lax.dot_general(
                queries, key_rows, (((1,), (1,)), ((), ())), preferred_element_type=jnp.float32
            ) * np.float32(HEAD_SIZE**-0.5)
            scores = jnp.where(allowed, scores, -1e30)
            weights = jnp.exp(scores - jnp.max(scores, axis=-1, keepdims=True))
            inverse = 1.0 / jnp.sum(weights, axis=-1, keepdims=True)
            probabilities = (weights * inverse).astype(jnp.bfloat16)
            attended = jnp.dot(
                probabilities, value_rows, preferred_element_type=jnp.float32
            ).astype(jnp.bfloat16)
            for j in range(per_tile):
                target = lax.rem(me - shift_ref[tile * per_tile + j] + senders, senders)
                for n in range(QUERY_PER_KEY):
                    column = (group * QUERY_PER_KEY + n) * HEAD_SIZE
                    out_ref[target, :, column : column + HEAD_SIZE] = attended[
                        n * TILE + j * IMG_MAX : n * TILE + (j + 1) * IMG_MAX, :
                    ]

    product(0)
    for group in range(1, len(heads)):
        product(group)
        attention(group - 1)
    attention(len(heads) - 1)


def attend(shift, hidden, rms_gain, w_qkv, part, square, senders):
    rows, depth = hidden.shape
    block = (QUERY_PER_KEY + 2) * HEAD_SIZE
    groups = w_qkv.shape[1] // block
    out_columns = groups * QUERY_PER_KEY * HEAD_SIZE
    cos, sine = rotary_tables()
    return pl.pallas_call(
        attend_body,
        in_specs=[SCALARS] + [WHOLE] * 7,
        out_specs=WHOLE,
        scratch_shapes=[
            pltpu.VMEM((rows, depth), jnp.bfloat16),
            pltpu.VMEM((rows, HEAD_SIZE), jnp.float32),
        ]
        + [pltpu.VMEM((rows, block), jnp.float32)] * groups,
        out_shape=jax.ShapeDtypeStruct((senders, IMG_MAX, out_columns), jnp.bfloat16),
        compiler_params=limit(10),
        cost_estimate=pl.CostEstimate(
            flops=2 * rows * depth * groups * block,
            bytes_accessed=2 * depth * groups * block,
            transcendentals=0,
        ),
        name="attend",
    )(shift, hidden, rms_gain, w_qkv, part, square, jnp.asarray(cos), jnp.asarray(sine))


def place_body(counts_ref, shift_ref, box_ref, out_ref):
    senders = box_ref.shape[0]
    per_tile = counts_ref.shape[0]
    tiles = shift_ref.shape[0] // per_tile
    me = lax.axis_index("dp")
    lane = lax.broadcasted_iota(jnp.int32, (TILE, TILE), 1)
    row = lax.broadcasted_iota(jnp.int32, (TILE, TILE), 0)
    inside = jnp.bitwise_and(lane, IMG_MAX - 1)
    image = lane // IMG_MAX
    for tile in range(tiles):
        goal = jnp.full((TILE, TILE), -1, jnp.int32)
        offset = jnp.int32(0)
        blocks = []
        for j in range(per_tile):
            count = counts_ref[j, me * tiles + tile]
            goal = jnp.where((image == j) & (inside < count), inside + offset, goal)
            offset = offset + count
            source = lax.rem(me + shift_ref[tile * per_tile + j], senders)
            blocks.append(box_ref[source])
        out_ref[tile * TILE : (tile + 1) * TILE, :] = jnp.dot(
            jnp.where(row == goal, 1.0, 0.0).astype(jnp.bfloat16),
            jnp.concatenate(blocks, axis=0),
            preferred_element_type=jnp.float32,
        ).astype(jnp.bfloat16)


def place_rows(counts, shift, box):
    senders, depth, columns = box.shape
    rows = shift.shape[0] * depth
    return pl.pallas_call(
        place_body,
        in_specs=[SCALARS] * 2 + [WHOLE],
        out_specs=WHOLE,
        out_shape=jax.ShapeDtypeStruct((rows, columns), jnp.bfloat16),
        compiler_params=limit(8),
        name="place_rows",
    )(counts, shift, box)


def local(
    patches, ln_gain, ln_bias, w_proj, proj_bias, rms_gain, w_qkv, image_counts, source_shift
):
    senders = lax.axis_size("dp")
    counts = image_counts.T
    other = lax.ppermute(patches, "mp", SWAP)
    own = layer_norm(patches, ln_gain, ln_bias)
    hidden = project(
        counts, source_shift, own, other, ln_gain, ln_bias, w_proj, proj_bias.reshape(1, -1)
    )
    far_hidden = lax.ppermute(hidden, "mp", SWAP)
    rms_row = rms_gain.reshape(1, -1)
    part, square = first_half(hidden, rms_row, w_qkv)
    outbox = attend(source_shift, far_hidden, rms_row, w_qkv, part, square, senders)
    in_box = lax.all_to_all(outbox, "dp", split_axis=0, concat_axis=0, tiled=True)
    return place_rows(counts, source_shift, in_box)


def solution(mesh):
    in_specs = (
        P(("dp", "mp"), None),
        P(),
        P(),
        P(None, "mp"),
        P("mp"),
        P(),
        P(None, "mp"),
        P(),
        P(),
    )
    out_specs = P("dp", "mp")
    return jax.shard_map(local, mesh=mesh, in_specs=in_specs, out_specs=out_specs, check_vma=False)
```

```python
import functools

import jax
import jax.numpy as jnp
import numpy as np
from jax import lax
from jax.experimental import pallas as pl
from jax.experimental.pallas import tpu as pltpu
from jax.sharding import PartitionSpec as P

HEAD_SIZE = 128
TILE = 128
QUERY_PER_KEY = 4
IMG_MAX = 16

norm_epsilon = 1e-05
rms_epsilon = 1e-05
rotary_base = 500000.0

SWAP = [(0, 1), (1, 0)]


WHOLE = pl.BlockSpec(memory_space=pltpu.VMEM)
SCALARS = pl.BlockSpec(memory_space=pltpu.SMEM)
FAR_MEMORY = pl.BlockSpec(memory_space=pltpu.HBM)
NORM_ROWS = 32
COLUMNS = 256
ROW_BOUNDS = (352, 384)


def limit(mib):
    return pltpu.CompilerParams(vmem_limit_bytes=mib * 1024 * 1024)


def rotary_tables(rows):
    half = HEAD_SIZE // 2
    frequency = rotary_base ** (-(np.arange(half, dtype=np.float64) * (2.0 / HEAD_SIZE)))
    angles = np.arange(rows, dtype=np.float64)[:, None] * frequency[None, :]
    cos = np.concatenate([np.cos(angles), np.cos(angles)], axis=-1)
    sine = np.concatenate([-np.sin(angles), np.sin(angles)], axis=-1)
    return jnp.asarray(cos.astype(np.float32)), jnp.asarray(sine.astype(np.float32))


def image_starts(counts_ref, shift_ref):
    images = shift_ref.shape[0]
    tile_images = counts_ref.shape[0]
    tiles = images // tile_images
    senders = counts_ref.shape[1] // tiles
    me = lax.axis_index("dp")
    starts = []
    start = jnp.int32(0)
    for k in range(images):
        starts.append(start)
        target = lax.rem(me - shift_ref[k] + senders, senders)
        start = start + counts_ref[k % tile_images, target * tiles + k // tile_images]
    return starts, start


def for_row_bound(total, most, run):
    below = jnp.int32(-1)
    for bound in (*ROW_BOUNDS, most):
        pl.when((total > below) & (total <= bound))(functools.partial(run, bound))
        below = jnp.int32(bound)


def normalised(rows, gain, bias):
    values = rows.astype(jnp.float32)
    width = values.shape[-1]
    row_mean = jnp.sum(values, axis=-1, keepdims=True) * (1.0 / width)
    centred = values - row_mean
    row_var = jnp.sum(centred * centred, axis=-1, keepdims=True) * (1.0 / width)
    scaled = centred * lax.rsqrt(row_var + norm_epsilon) * gain.astype(jnp.float32)
    return (scaled + bias.astype(jnp.float32)).astype(jnp.bfloat16)


def fill_normed(src_ref, gain, bias, dst_ref, first, count, base):
    def fill(i, carry):
        src = pl.multiple_of(first + i * NORM_ROWS, NORM_ROWS)
        dst = pl.multiple_of(base + first + i * NORM_ROWS, NORM_ROWS)
        dst_ref[pl.ds(dst, NORM_ROWS), :] = normalised(
            src_ref[pl.ds(src, NORM_ROWS), :], gain, bias
        )
        return carry

    lax.fori_loop(0, count // NORM_ROWS, fill, 0)


NORM_PARTS = 4


def norm_own_body(rows_hbm, gain_hbm, bias_hbm, out_ref, rows_ref, gain_ref, bias_ref, sems):
    count, width = rows_ref.shape
    part = count // NORM_PARTS
    small = [
        pltpu.make_async_copy(gain_hbm, gain_ref, sems.at[NORM_PARTS]),
        pltpu.make_async_copy(bias_hbm, bias_ref, sems.at[NORM_PARTS + 1]),
    ]
    parts = [
        pltpu.make_async_copy(
            rows_hbm.at[pl.ds(n * part, part)], rows_ref.at[pl.ds(n * part, part)], sems.at[n]
        )
        for n in range(NORM_PARTS)
    ]
    for copy in small + parts:
        copy.start()
    for copy in small:
        copy.wait()
    gain = gain_ref[...].reshape(1, width)
    bias = bias_ref[...].reshape(1, width)
    for n in range(NORM_PARTS):
        parts[n].wait()
        fill_normed(rows_ref, gain, bias, out_ref, n * part, part, 0)


def norm_own(rows, gain, bias):
    count, width = rows.shape
    return pl.pallas_call(
        norm_own_body,
        in_specs=[FAR_MEMORY] * 3,
        out_specs=WHOLE,
        out_shape=jax.ShapeDtypeStruct((count, width), jnp.bfloat16),
        scratch_shapes=[
            pltpu.VMEM((count, width), jnp.bfloat16),
            pltpu.VMEM((width,), jnp.bfloat16),
            pltpu.VMEM((width,), jnp.bfloat16),
            pltpu.SemaphoreType.DMA((NORM_PARTS + 2,)),
        ],
        compiler_params=limit(8),
        cost_estimate=pl.CostEstimate(
            flops=8_000_000_000, bytes_accessed=4 * count * width, transcendentals=0
        ),
        name="norm_own",
    )(rows, gain, bias)


def norm_other_body(own_ref, other_ref, gain_ref, bias_ref, out_ref):
    half, width = own_ref.shape
    core = lax.axis_index("mp")
    out_ref[pl.ds(pl.multiple_of(core * half, half), half), :] = own_ref[...]
    fill_normed(
        other_ref, gain_ref[...].reshape(1, width), bias_ref[...].reshape(1, width), out_ref,
        0, half, pl.multiple_of((1 - core) * half, half),
    )


def norm_other(own, other, gain, bias):
    half, width = own.shape
    return pl.pallas_call(
        norm_other_body,
        in_specs=[WHOLE] * 4,
        out_specs=WHOLE,
        out_shape=jax.ShapeDtypeStruct((2 * half, width), jnp.bfloat16),
        compiler_params=limit(6),
        cost_estimate=pl.CostEstimate(
            flops=10 * half * width, bytes_accessed=4 * half * width, transcendentals=0
        ),
        name="norm_other",
    )(own, other, gain, bias)


def project_body(
    counts_ref, shift_ref, normed_ref, w_ref, add_ref, rms_ref,
    out_ref, add_row, rms_row, squares, acc_even, acc_odd,
):
    rows = normed_ref.shape[0]
    columns = w_ref.shape[1]
    blocks = columns // COLUMNS
    total = image_starts(counts_ref, shift_ref)[1]
    mine = pl.multiple_of(lax.axis_index("mp") * columns, columns)
    add_row[...] = add_ref[...].reshape(1, columns).astype(jnp.float32)
    rms_row[...] = rms_ref[...].reshape(1, 2 * columns).astype(jnp.float32)
    acc_odd[...] = jnp.zeros_like(acc_odd)

    def run(bound):
        used = pl.ds(0, bound)

        def product(block, acc):
            at = pl.multiple_of(block * COLUMNS, COLUMNS)
            acc[used, :] = jnp.dot(
                normed_ref[used, :], w_ref[:, pl.ds(at, COLUMNS)],
                preferred_element_type=jnp.float32,
            )

        def post(block, acc, keep=None):
            at = pl.multiple_of(block * COLUMNS, COLUMNS)
            pre = acc[used, :] + add_row[:, pl.ds(at, COLUMNS)]
            value = pre * (1.0 + lax.erf(pre * np.float32(0.5**0.5))) * 0.5
            value = value.astype(jnp.bfloat16).astype(jnp.float32)
            gain = rms_row[:, pl.ds(pl.multiple_of(mine + at, COLUMNS), COLUMNS)]
            out_ref[used, pl.ds(at, COLUMNS)] = (value * gain).astype(jnp.bfloat16)
            square = value[:, :128] * value[:, :128] + value[:, 128:] * value[:, 128:]
            if keep is not None:
                square = jnp.where(keep, square, 0.0)
            squares[used, :] = squares[used, :] + square

        squares[...] = jnp.zeros_like(squares)

        def pair(p, carry):
            product(2 * p, acc_even)
            post(jnp.maximum(2 * p - 1, 0), acc_odd, p > 0)
            product(2 * p + 1, acc_odd)
            post(2 * p, acc_even)
            return carry

        lax.fori_loop(0, blocks // 2, pair, 0)
        post(blocks - 1, acc_odd)
        row_sum = jnp.sum(squares[used, :], axis=-1, keepdims=True)
        high = row_sum.astype(jnp.bfloat16).astype(jnp.float32)
        lane = lax.broadcasted_iota(jnp.int32, (bound, 128), 1)
        out_ref[used, columns : columns + 128] = jnp.where(
            lane < 64, high, row_sum - high
        ).astype(jnp.bfloat16)

    for_row_bound(total, rows, run)


def project(counts, shift, normed, w_proj, proj_bias, rms_gain):
    rows, width = normed.shape
    columns = w_proj.shape[1]
    return pl.pallas_call(
        project_body,
        in_specs=[SCALARS] * 2 + [WHOLE] * 4,
        out_specs=WHOLE,
        scratch_shapes=[
            pltpu.VMEM((1, columns), jnp.float32),
            pltpu.VMEM((1, 2 * columns), jnp.float32),
            pltpu.VMEM((rows, 128), jnp.float32),
            pltpu.VMEM((rows, COLUMNS), jnp.float32),
            pltpu.VMEM((rows, COLUMNS), jnp.float32),
        ],
        out_shape=jax.ShapeDtypeStruct((rows, columns + 128), jnp.bfloat16),
        compiler_params=limit(8),
        cost_estimate=pl.CostEstimate(
            flops=2 * rows * width * columns,
            bytes_accessed=2 * width * columns,
            transcendentals=rows * columns,
        ),
        name="project",
    )(counts, shift, normed, w_proj, proj_bias, rms_gain)


def first_half_body(counts_ref, shift_ref, gained_ref, w_ref, part_ref):
    rows = gained_ref.shape[0]
    depth = w_ref.shape[0] // 2
    mine = pl.multiple_of(lax.axis_index("mp") * depth, depth)
    total = image_starts(counts_ref, shift_ref)[1]

    def run(bound):
        def block(j, carry):
            at = pl.multiple_of(j * COLUMNS, COLUMNS)
            part_ref[pl.ds(0, bound), pl.ds(at, COLUMNS)] = jnp.dot(
                gained_ref[pl.ds(0, bound), pl.ds(0, depth)],
                w_ref[pl.ds(mine, depth), pl.ds(at, COLUMNS)],
                preferred_element_type=jnp.float32,
            )
            return carry

        lax.fori_loop(0, w_ref.shape[1] // COLUMNS, block, 0)

    for_row_bound(total, rows, run)


def first_half(counts, shift, gained, w_qkv):
    rows = gained.shape[0]
    depth, columns = w_qkv.shape
    return pl.pallas_call(
        first_half_body,
        in_specs=[SCALARS] * 2 + [WHOLE] * 2,
        out_specs=WHOLE,
        out_shape=jax.ShapeDtypeStruct((rows, columns), jnp.float32),
        compiler_params=limit(6),
        cost_estimate=pl.CostEstimate(
            flops=rows * depth * columns,
            bytes_accessed=depth * columns + 4 * rows * columns,
            transcendentals=0,
        ),
        name="first_half",
    )(counts, shift, gained, w_qkv)


def attend_body(
    counts_ref, shift_ref, near_ref, far_ref, w_ref, part_ref, cos_ref, sine_ref,
    out_ref, align, factor, turned_rows, slots, *heads,
):
    rows = far_ref.shape[0]
    depth = w_ref.shape[0] // 2
    senders = out_ref.shape[0]
    per_tile = TILE // IMG_MAX
    width = heads[0].shape[1]
    me = lax.axis_index("dp")
    far = pl.multiple_of((1 - lax.axis_index("mp")) * depth, depth)
    starts, total = image_starts(counts_ref, shift_ref)
    column = lax.broadcasted_iota(jnp.int32, (IMG_MAX, rows), 1)
    distance = column - lax.broadcasted_iota(jnp.int32, (IMG_MAX, rows), 0)
    for k, start in enumerate(starts):
        align[k * IMG_MAX : (k + 1) * IMG_MAX, :] = jnp.where(distance == start, 1.0, 0.0).astype(
            jnp.bfloat16
        )
    q_at = lax.broadcasted_iota(jnp.int32, (QUERY_PER_KEY * TILE, TILE), 0)
    k_at = lax.broadcasted_iota(jnp.int32, (QUERY_PER_KEY * TILE, TILE), 1)
    q_at = jnp.bitwise_and(q_at, TILE - 1)
    allowed = (q_at >= k_at) & ((q_at // IMG_MAX) == (k_at // IMG_MAX))

    def run(bound):
        used = slice(0, bound)
        both = near_ref[used, depth:].astype(jnp.float32) + far_ref[used, depth:].astype(
            jnp.float32
        )
        squares = both[:, 0:1] + both[:, 64:65]
        factor[used, :] = jnp.broadcast_to(
            lax.rsqrt(squares * (1.0 / (2 * depth)) + rms_epsilon), (bound, HEAD_SIZE)
        )

        def product(group):
            at = slice(group * width, (group + 1) * width)
            heads[group][used, :] = part_ref[used, at] + jnp.dot(
                far_ref[used, 0:depth], w_ref[pl.ds(far, depth), at],
                preferred_element_type=jnp.float32,
            )

        def attention(group):
            for n in range(QUERY_PER_KEY + 2):
                at = slice(n * HEAD_SIZE, (n + 1) * HEAD_SIZE)
                values = heads[group][used, at] * factor[used, :]
                if n <= QUERY_PER_KEY:
                    turned = pltpu.roll(values, HEAD_SIZE // 2, 1)
                    values = values * cos_ref[used, :] + turned * sine_ref[used, :]
                turned_rows[used, at] = values.astype(jnp.bfloat16)
            slots[...] = jnp.dot(
                align[:, used], turned_rows[used, :], preferred_element_type=jnp.float32
            ).astype(jnp.bfloat16)
            for tile in range(rows // TILE):
                at = slice(tile * TILE, (tile + 1) * TILE)

                def head(n):
                    return slots[at, n * HEAD_SIZE : (n + 1) * HEAD_SIZE]

                queries = jnp.concatenate([head(n) for n in range(QUERY_PER_KEY)], axis=0)
                scores = lax.dot_general(
                    queries, head(QUERY_PER_KEY), (((1,), (1,)), ((), ())),
                    preferred_element_type=jnp.float32,
                )
                scores = jnp.where(allowed, scores * np.float32(HEAD_SIZE**-0.5), -1e30)
                weights = jnp.exp(scores - jnp.max(scores, axis=-1, keepdims=True))
                inverse = 1.0 / jnp.sum(weights, axis=-1, keepdims=True)
                attended = jnp.dot(
                    (weights * inverse).astype(jnp.bfloat16), head(QUERY_PER_KEY + 1),
                    preferred_element_type=jnp.float32,
                ).astype(jnp.bfloat16)
                for j in range(per_tile):
                    target = lax.rem(me - shift_ref[tile * per_tile + j] + senders, senders)
                    for n in range(QUERY_PER_KEY):
                        column = (group * QUERY_PER_KEY + n) * HEAD_SIZE
                        out_ref[target, :, column : column + HEAD_SIZE] = attended[
                            n * TILE + j * IMG_MAX : n * TILE + (j + 1) * IMG_MAX, :
                        ]

        product(0)
        for group in range(1, len(heads)):
            product(group)
            attention(group - 1)
        attention(len(heads) - 1)

    for_row_bound(total, rows, run)


def attend(counts, shift, near, far, w_qkv, part, senders):
    rows = far.shape[0]
    block = (QUERY_PER_KEY + 2) * HEAD_SIZE
    depth, columns = w_qkv.shape
    groups = columns // block
    out_columns = groups * QUERY_PER_KEY * HEAD_SIZE
    cos, sine = rotary_tables(rows)
    return pl.pallas_call(
        attend_body,
        in_specs=[SCALARS] * 2 + [WHOLE] * 6,
        out_specs=WHOLE,
        scratch_shapes=[
            pltpu.VMEM((rows, rows), jnp.bfloat16),
            pltpu.VMEM((rows, HEAD_SIZE), jnp.float32),
            pltpu.VMEM((rows, block), jnp.bfloat16),
            pltpu.VMEM((rows, block), jnp.bfloat16),
        ]
        + [pltpu.VMEM((rows, block), jnp.float32)] * groups,
        out_shape=jax.ShapeDtypeStruct((senders, IMG_MAX, out_columns), jnp.bfloat16),
        compiler_params=limit(12),
        cost_estimate=pl.CostEstimate(
            flops=rows * depth * columns, bytes_accessed=depth * columns, transcendentals=0
        ),
        name="attend",
    )(counts, shift, near, far, w_qkv, part, cos, sine)


def place_body(counts_ref, shift_ref, box_ref, out_hbm, placed, sems):
    senders = box_ref.shape[0]
    per_tile = counts_ref.shape[0]
    tiles = shift_ref.shape[0] // per_tile
    me = lax.axis_index("dp")
    lane = lax.broadcasted_iota(jnp.int32, (TILE, TILE), 1)
    row = lax.broadcasted_iota(jnp.int32, (TILE, TILE), 0)
    inside = jnp.bitwise_and(lane, IMG_MAX - 1)
    image = lane // IMG_MAX
    copies = []
    for tile in range(tiles):
        goal = jnp.full((TILE, TILE), -1, jnp.int32)
        offset = jnp.int32(0)
        blocks = []
        for j in range(per_tile):
            count = counts_ref[j, me * tiles + tile]
            goal = jnp.where((image == j) & (inside < count), inside + offset, goal)
            offset = offset + count
            source = lax.rem(me + shift_ref[tile * per_tile + j], senders)
            blocks.append(box_ref[source])
        at = pl.ds(tile * TILE, TILE)
        placed[at, :] = jnp.dot(
            jnp.where(row == goal, 1.0, 0.0).astype(jnp.bfloat16),
            jnp.concatenate(blocks, axis=0),
            preferred_element_type=jnp.float32,
        ).astype(jnp.bfloat16)
        copy = pltpu.make_async_copy(placed.at[at], out_hbm.at[at], sems.at[tile])
        copy.start()
        copies.append(copy)
    for copy in copies:
        copy.wait()


def place_rows(counts, shift, box):
    senders, depth, columns = box.shape
    rows = shift.shape[0] * depth
    return pl.pallas_call(
        place_body,
        in_specs=[SCALARS] * 2 + [WHOLE],
        out_specs=FAR_MEMORY,
        out_shape=jax.ShapeDtypeStruct((rows, columns), jnp.bfloat16),
        scratch_shapes=[
            pltpu.VMEM((rows, columns), jnp.bfloat16),
            pltpu.SemaphoreType.DMA((rows // TILE,)),
        ],
        compiler_params=limit(8),
        name="place_rows",
    )(counts, shift, box)


def local(
    patches, ln_gain, ln_bias, w_proj, proj_bias, rms_gain, w_qkv, image_counts, source_shift
):
    senders = lax.axis_size("dp")
    counts = image_counts.T
    other = lax.ppermute(patches, "mp", SWAP)
    pin = lambda x: pltpu.with_memory_space_constraint(x, pltpu.HBM)
    own = norm_own(pin(patches), pin(ln_gain), pin(ln_bias))
    normed = norm_other(own, other, ln_gain, ln_bias)
    near = project(counts, source_shift, normed, w_proj, proj_bias, rms_gain)
    far = lax.ppermute(near, "mp", SWAP)
    part = first_half(counts, source_shift, near, w_qkv)
    outbox = attend(counts, source_shift, near, far, w_qkv, part, senders)
    in_box = lax.all_to_all(outbox, "dp", split_axis=0, concat_axis=0, tiled=True)
    return place_rows(counts, source_shift, in_box)


def solution(mesh):
    in_specs = (
        P(("dp", "mp"), None),
        P(),
        P(),
        P(None, "mp"),
        P("mp"),
        P(),
        P(None, "mp"),
        P(),
        P(),
    )
    out_specs = P("dp", "mp")
    return jax.shard_map(local, mesh=mesh, in_specs=in_specs, out_specs=out_specs, check_vma=False)
```

```python
import functools

import jax
import jax.numpy as jnp
import numpy as np
from jax import lax
from jax.experimental import pallas as pl
from jax.experimental.pallas import tpu as pltpu
from jax.sharding import PartitionSpec as P

HEAD_SIZE = 128
TILE = 128
QUERY_PER_KEY = 4
IMG_MAX = 16

norm_epsilon = 1e-05
rms_epsilon = 1e-05
rotary_base = 500000.0

SWAP = [(0, 1), (1, 0)]


WHOLE = pl.BlockSpec(memory_space=pltpu.VMEM)
SCALARS = pl.BlockSpec(memory_space=pltpu.SMEM)
FAR_MEMORY = pl.BlockSpec(memory_space=pltpu.HBM)
NORM_ROWS = 32
CUTS = (1024, 768, 256)
NARROW = 256
QKV_COLUMNS = 768
WINDOW = TILE + 2 * IMG_MAX
ROW_BOUNDS = (352, 384)


def limit(mib):
    return pltpu.CompilerParams(vmem_limit_bytes=mib * 1024 * 1024)


def rotary_tables(rows):
    half = HEAD_SIZE // 2
    frequency = rotary_base ** (-(np.arange(half, dtype=np.float64) * (2.0 / HEAD_SIZE)))
    angles = np.arange(rows, dtype=np.float64)[:, None] * frequency[None, :]
    cos = np.concatenate([np.cos(angles), np.cos(angles)], axis=-1)
    sine = np.concatenate([-np.sin(angles), np.sin(angles)], axis=-1)
    return jnp.asarray(cos.astype(np.float32)), jnp.asarray(sine.astype(np.float32))


def write_plan(counts_ref, shift_ref, plan_ref):
    images = shift_ref.shape[0]
    tile_images = counts_ref.shape[0]
    tiles = images // tile_images
    senders = counts_ref.shape[1] // tiles
    me = lax.axis_index("dp")
    start = jnp.int32(0)
    for k in range(images):
        plan_ref[k] = start
        target = lax.rem(me - shift_ref[k] + senders, senders)
        plan_ref[images + 1 + k] = target
        start = start + counts_ref[k % tile_images, target * tiles + k // tile_images]
    plan_ref[images] = start


def for_row_bound(total, most, run):
    below = jnp.int32(-1)
    for bound in (*ROW_BOUNDS, most):
        pl.when((total > below) & (total <= bound))(functools.partial(run, bound))
        below = jnp.int32(bound)


def normalised(rows, gain, bias):
    values = rows.astype(jnp.float32)
    width = values.shape[-1]
    row_mean = jnp.sum(values, axis=-1, keepdims=True) * (1.0 / width)
    centred = values - row_mean
    row_var = jnp.sum(centred * centred, axis=-1, keepdims=True) * (1.0 / width)
    scaled = centred * lax.rsqrt(row_var + norm_epsilon) * gain
    return (scaled + bias).astype(jnp.bfloat16)


def fill_normed(src_ref, gain_row, bias_row, dst_ref, first, count, base):
    def fill(i, carry):
        src = pl.multiple_of(first + i * NORM_ROWS, NORM_ROWS)
        dst = pl.multiple_of(base + first + i * NORM_ROWS, NORM_ROWS)
        dst_ref[pl.ds(dst, NORM_ROWS), :] = normalised(
            src_ref[pl.ds(src, NORM_ROWS), :], gain_row[...], bias_row[...]
        )
        return carry

    lax.fori_loop(0, count // NORM_ROWS, fill, 0, unroll=2)


NORM_PARTS = 4


def norm_own_body(rows_hbm, gain_hbm, bias_hbm, out_ref, rows_ref, gain_ref, bias_ref, gain_row, bias_row, sems):
    count, width = rows_ref.shape
    part = count // NORM_PARTS
    small = [
        pltpu.make_async_copy(gain_hbm, gain_ref, sems.at[NORM_PARTS]),
        pltpu.make_async_copy(bias_hbm, bias_ref, sems.at[NORM_PARTS + 1]),
    ]
    parts = [
        pltpu.make_async_copy(
            rows_hbm.at[pl.ds(n * part, part)], rows_ref.at[pl.ds(n * part, part)], sems.at[n]
        )
        for n in range(NORM_PARTS)
    ]
    for copy in small + parts:
        copy.start()
    for copy in small:
        copy.wait()
    gain_row[...] = gain_ref[...].reshape(1, width).astype(jnp.float32)
    bias_row[...] = bias_ref[...].reshape(1, width).astype(jnp.float32)
    for n in range(NORM_PARTS):
        parts[n].wait()
        fill_normed(rows_ref, gain_row, bias_row, out_ref, n * part, part, 0)


def norm_own(rows, gain, bias):
    count, width = rows.shape
    return pl.pallas_call(
        norm_own_body,
        in_specs=[FAR_MEMORY] * 3,
        out_specs=WHOLE,
        out_shape=jax.ShapeDtypeStruct((count, width), jnp.bfloat16),
        scratch_shapes=[
            pltpu.VMEM((count, width), jnp.bfloat16),
            pltpu.VMEM((width,), jnp.bfloat16),
            pltpu.VMEM((width,), jnp.bfloat16),
            pltpu.VMEM((1, width), jnp.float32),
            pltpu.VMEM((1, width), jnp.float32),
            pltpu.SemaphoreType.DMA((NORM_PARTS + 2,)),
        ],
        compiler_params=limit(8),
        cost_estimate=pl.CostEstimate(
            flops=8_000_000_000, bytes_accessed=4 * count * width, transcendentals=0
        ),
        name="norm_own",
    )(rows, gain, bias)


def norm_other_body(
    counts_ref, shift_ref, own_ref, other_ref, gain_ref, bias_ref, out_ref, plan_ref,
    gain_row, bias_row,
):
    write_plan(counts_ref, shift_ref, plan_ref)
    half, width = own_ref.shape
    core = lax.axis_index("mp")
    out_ref[pl.ds(pl.multiple_of(core * half, half), half), :] = own_ref[...]
    gain_row[...] = gain_ref[...].reshape(1, width).astype(jnp.float32)
    bias_row[...] = bias_ref[...].reshape(1, width).astype(jnp.float32)
    fill_normed(
        other_ref, gain_row, bias_row, out_ref, 0, half, pl.multiple_of((1 - core) * half, half)
    )


def norm_other(counts, shift, own, other, gain, bias):
    half, width = own.shape
    images = shift.shape[0]
    return pl.pallas_call(
        norm_other_body,
        in_specs=[SCALARS] * 2 + [WHOLE] * 4,
        out_specs=[WHOLE, SCALARS],
        out_shape=[
            jax.ShapeDtypeStruct((2 * half, width), jnp.bfloat16),
            jax.ShapeDtypeStruct((2 * images + 1,), jnp.int32),
        ],
        scratch_shapes=[pltpu.VMEM((1, width), jnp.float32)] * 2,
        compiler_params=limit(6),
        cost_estimate=pl.CostEstimate(
            flops=10 * half * width, bytes_accessed=4 * half * width, transcendentals=0
        ),
        name="norm_other",
    )(counts, shift, own, other, gain, bias)


def project_body(
    plan_ref, normed_ref, w_ref, add_ref, rms_ref,
    out_ref, add_row, rms_row, squares, acc_even, acc_odd,
):
    rows = normed_ref.shape[0]
    columns = w_ref.shape[1]
    total = plan_ref[plan_ref.shape[0] // 2]
    mine = pl.multiple_of(lax.axis_index("mp") * columns, columns)
    add_row[...] = add_ref[...].reshape(1, columns).astype(jnp.float32)
    rms_row[...] = rms_ref[...].reshape(1, 2 * columns).astype(jnp.float32)

    def run(bound):
        used = pl.ds(0, bound)

        def product(first, width, acc):
            acc[used, 0:width] = jnp.dot(
                normed_ref[used, :], w_ref[:, pl.ds(first, width)],
                preferred_element_type=jnp.float32,
            )

        def post(first, width, acc):
            pre = acc[used, 0:width] + add_row[:, pl.ds(first, width)]
            value = pre * (1.0 + lax.erf(pre * np.float32(0.5**0.5))) * 0.5
            value = value.astype(jnp.bfloat16).astype(jnp.float32)
            gain = rms_row[:, pl.ds(pl.multiple_of(mine + first, NARROW), width)]
            out_ref[used, pl.ds(first, width)] = (value * gain).astype(jnp.bfloat16)
            square = sum(
                value[:, c : c + 128] * value[:, c : c + 128] for c in range(0, width, 128)
            )
            squares[used, :] = squares[used, :] + square

        squares[...] = jnp.zeros_like(squares)
        if bound < rows:
            first, waiting = 0, None
            for n, width in enumerate(CUTS):
                acc = (acc_even, acc_odd)[n % 2]
                product(first, width, acc)
                if waiting is not None:
                    post(*waiting)
                waiting = (first, width, acc)
                first += width
            post(*waiting)
        else:

            def block(n, carry):
                at = pl.multiple_of(n * NARROW, NARROW)
                product(at, NARROW, acc_even)
                post(at, NARROW, acc_even)
                return carry

            lax.fori_loop(0, columns // NARROW, block, 0)
        row_sum = jnp.sum(squares[used, :], axis=-1, keepdims=True)
        high = row_sum.astype(jnp.bfloat16).astype(jnp.float32)
        lane = lax.broadcasted_iota(jnp.int32, (bound, 128), 1)
        out_ref[used, columns : columns + 128] = jnp.where(
            lane < 64, high, row_sum - high
        ).astype(jnp.bfloat16)

    for_row_bound(total, rows, run)


def project(plan, normed, w_proj, proj_bias, rms_gain):
    rows, width = normed.shape
    columns = w_proj.shape[1]
    return pl.pallas_call(
        project_body,
        in_specs=[SCALARS] + [WHOLE] * 4,
        out_specs=WHOLE,
        scratch_shapes=[
            pltpu.VMEM((1, columns), jnp.float32),
            pltpu.VMEM((1, 2 * columns), jnp.float32),
            pltpu.VMEM((rows, 128), jnp.float32),
            pltpu.VMEM((rows, CUTS[0]), jnp.float32),
            pltpu.VMEM((rows, CUTS[1]), jnp.float32),
        ],
        out_shape=jax.ShapeDtypeStruct((rows, columns + 128), jnp.bfloat16),
        compiler_params=limit(18),
        cost_estimate=pl.CostEstimate(
            flops=2 * rows * width * columns,
            bytes_accessed=2 * width * columns,
            transcendentals=rows * columns,
        ),
        name="project",
    )(plan, normed, w_proj, proj_bias, rms_gain)


def first_half_body(plan_ref, gained_ref, w_ref, part_ref):
    rows = gained_ref.shape[0]
    depth = w_ref.shape[0] // 2
    mine = pl.multiple_of(lax.axis_index("mp") * depth, depth)
    total = plan_ref[plan_ref.shape[0] // 2]

    def run(bound):
        def block(j, carry):
            at = pl.multiple_of(j * QKV_COLUMNS, QKV_COLUMNS)
            part_ref[pl.ds(0, bound), pl.ds(at, QKV_COLUMNS)] = jnp.dot(
                gained_ref[pl.ds(0, bound), pl.ds(0, depth)],
                w_ref[pl.ds(mine, depth), pl.ds(at, QKV_COLUMNS)],
                preferred_element_type=jnp.float32,
            )
            return carry

        lax.fori_loop(0, w_ref.shape[1] // QKV_COLUMNS, block, 0)

    for_row_bound(total, rows, run)


def first_half(plan, gained, w_qkv):
    rows = gained.shape[0]
    depth, columns = w_qkv.shape
    return pl.pallas_call(
        first_half_body,
        in_specs=[SCALARS] + [WHOLE] * 2,
        out_specs=WHOLE,
        out_shape=jax.ShapeDtypeStruct((rows, columns), jnp.float32),
        compiler_params=limit(6),
        cost_estimate=pl.CostEstimate(
            flops=rows * depth * columns,
            bytes_accessed=depth * columns + 4 * rows * columns,
            transcendentals=0,
        ),
        name="first_half",
    )(plan, gained, w_qkv)


def attend_body(
    plan_ref, near_ref, far_ref, w_ref, part_ref, cos_ref, sine_ref,
    out_ref, factor, ones, align, heads, turned_rows, queries, keys, values, scores,
):
    groups, padded, width = turned_rows.shape
    rows = far_ref.shape[0]
    depth = w_ref.shape[0] // 2
    images = plan_ref.shape[0] // 2
    per_tile = TILE // IMG_MAX
    tiles = rows // TILE
    pair = 2 * HEAD_SIZE
    far = pl.multiple_of((1 - lax.axis_index("mp")) * depth, depth)
    starts = [plan_ref[k] for k in range(images)]
    total = plan_ref[images]
    targets = [plan_ref[images + 1 + k] for k in range(images)]
    bases = [
        pl.multiple_of((starts[tile * per_tile] // IMG_MAX) * IMG_MAX, IMG_MAX)
        for tile in range(tiles)
    ]

    def prepare():
        column = lax.broadcasted_iota(jnp.int32, (IMG_MAX, WINDOW), 1)
        distance = column - lax.broadcasted_iota(jnp.int32, (IMG_MAX, WINDOW), 0)
        empty = jnp.zeros((groups, tiles, HEAD_SIZE, HEAD_SIZE), jnp.bfloat16)
        for tile in range(tiles):
            for j in range(per_tile):
                align[tile, j * IMG_MAX : (j + 1) * IMG_MAX, :] = jnp.where(
                    distance == starts[tile * per_tile + j] - bases[tile], 1.0, 0.0
                ).astype(jnp.bfloat16)
        for kept in (keys, values):
            kept[:, :, 0:HEAD_SIZE, HEAD_SIZE:pair] = empty
            kept[:, :, HEAD_SIZE:pair, 0:HEAD_SIZE] = empty
        side = lax.broadcasted_iota(jnp.int32, (pair, pair), 0) // HEAD_SIZE
        ones[...] = jnp.where(
            side == lax.broadcasted_iota(jnp.int32, (pair, pair), 1) // HEAD_SIZE, 1.0, 0.0
        ).astype(jnp.bfloat16)

    q_at = jnp.bitwise_and(lax.broadcasted_iota(jnp.int32, (pair, pair), 0), TILE - 1)
    k_at = jnp.bitwise_and(lax.broadcasted_iota(jnp.int32, (pair, pair), 1), TILE - 1)
    allowed = (q_at >= k_at) & ((q_at // IMG_MAX) == (k_at // IMG_MAX))

    def line_up(group):
        for tile in range(tiles):
            window = turned_rows[group, pl.ds(bases[tile], WINDOW), :]
            placed = jnp.dot(align[tile], window, preferred_element_type=jnp.float32).astype(
                jnp.bfloat16
            )
            queries[group, tile * TILE : (tile + 1) * TILE, :] = placed[:, 0 : 2 * pair]
            for kept, n in ((keys, QUERY_PER_KEY), (values, QUERY_PER_KEY + 1)):
                block = placed[:, n * HEAD_SIZE : (n + 1) * HEAD_SIZE]
                kept[group, tile, 0:TILE, 0:HEAD_SIZE] = block
                kept[group, tile, TILE : 2 * TILE, HEAD_SIZE:pair] = block

    def score(group):
        for tile in range(tiles):
            at = slice(tile * TILE, (tile + 1) * TILE)
            stacked = jnp.concatenate(
                [queries[group, at, 0:pair], queries[group, at, pair : 2 * pair]], axis=0
            )
            scores[group, tile] = lax.dot_general(
                stacked, keys[group, tile], (((1,), (1,)), ((), ())),
                preferred_element_type=jnp.float32,
            )

    def weigh(group):
        for tile in range(tiles):
            seen = jnp.where(allowed, scores[group, tile] * np.float32(HEAD_SIZE**-0.5), -1e30)
            weights = jnp.concatenate(
                [
                    jnp.exp(half - jnp.max(half, axis=-1, keepdims=True)).astype(jnp.bfloat16)
                    for half in (seen[:, 0:HEAD_SIZE], seen[:, HEAD_SIZE:pair])
                ],
                axis=1,
            )
            weighed = jnp.dot(weights, values[group, tile], preferred_element_type=jnp.float32)
            row_sum = jnp.dot(weights, ones[...], preferred_element_type=jnp.float32)
            attended = (weighed * (1.0 / row_sum)).astype(jnp.bfloat16)
            for j in range(per_tile):
                target = targets[tile * per_tile + j]
                for n in range(2):
                    column = group * QUERY_PER_KEY * HEAD_SIZE + n * pair
                    out_ref[target, :, column : column + pair] = attended[
                        n * TILE + j * IMG_MAX : n * TILE + (j + 1) * IMG_MAX, :
                    ]

    def run(bound):
        used = slice(0, bound)
        both = near_ref[used, depth:].astype(jnp.float32) + far_ref[used, depth:].astype(
            jnp.float32
        )
        squares = both[:, 0:1] + both[:, 64:65]
        factor[used, :] = jnp.broadcast_to(
            lax.rsqrt(squares * (1.0 / (2 * depth)) + rms_epsilon), (bound, HEAD_SIZE)
        )

        def piece(group, first, size):
            at = pl.ds(group * width + first, size)
            heads[group, used, pl.ds(first, size)] = part_ref[used, at] + jnp.dot(
                far_ref[used, 0:depth], w_ref[pl.ds(far, depth), at],
                preferred_element_type=jnp.float32,
            )

        def product(group, first, last):
            if bound < rows:
                piece(group, first, last - first)
            else:

                def narrow(n, carry):
                    piece(group, pl.multiple_of(first + n * NARROW, NARROW), NARROW)
                    return carry

                lax.fori_loop(0, (last - first) // NARROW, narrow, 0)

        def rotate(group):
            for n in range(QUERY_PER_KEY + 2):
                at = slice(n * HEAD_SIZE, (n + 1) * HEAD_SIZE)
                rows_in = heads[group, used, at] * factor[used, :]
                if n <= QUERY_PER_KEY:
                    turned = pltpu.roll(rows_in, HEAD_SIZE // 2, 1)
                    rows_in = rows_in * cos_ref[used, :] + turned * sine_ref[used, :]
                turned_rows[group, used, at] = rows_in.astype(jnp.bfloat16)

        product(0, 0, width)
        prepare()
        turned_rows[:, bound:, :] = jnp.zeros((groups, padded - bound, width), jnp.bfloat16)
        for group in range(1, groups):
            product(group, 0, 512)
            rotate(group - 1)
            line_up(group - 1)
            score(group - 1)
            product(group, 512, width)
            weigh(group - 1)
        rotate(groups - 1)
        line_up(groups - 1)
        score(groups - 1)
        weigh(groups - 1)

    for_row_bound(total, rows, run)


def attend(plan, near, far, w_qkv, part, senders):
    rows = far.shape[0]
    block = (QUERY_PER_KEY + 2) * HEAD_SIZE
    depth, columns = w_qkv.shape
    groups = columns // block
    out_columns = groups * QUERY_PER_KEY * HEAD_SIZE
    padded = rows + WINDOW
    pair = 2 * HEAD_SIZE
    tiles = rows // TILE
    cos, sine = rotary_tables(rows)
    return pl.pallas_call(
        attend_body,
        in_specs=[SCALARS] + [WHOLE] * 6,
        out_specs=WHOLE,
        scratch_shapes=[
            pltpu.VMEM((rows, HEAD_SIZE), jnp.float32),
            pltpu.VMEM((pair, pair), jnp.bfloat16),
            pltpu.VMEM((tiles, TILE, WINDOW), jnp.bfloat16),
            pltpu.VMEM((groups, rows, block), jnp.float32),
            pltpu.VMEM((groups, padded, block), jnp.bfloat16),
            pltpu.VMEM((groups, rows, 2 * pair), jnp.bfloat16),
            pltpu.VMEM((groups, tiles, pair, pair), jnp.bfloat16),
            pltpu.VMEM((groups, tiles, pair, pair), jnp.bfloat16),
            pltpu.VMEM((groups, tiles, pair, pair), jnp.float32),
        ],
        out_shape=jax.ShapeDtypeStruct((senders, IMG_MAX, out_columns), jnp.bfloat16),
        compiler_params=limit(20),
        cost_estimate=pl.CostEstimate(
            flops=rows * depth * columns, bytes_accessed=depth * columns, transcendentals=0
        ),
        name="attend",
    )(plan, near, far, w_qkv, part, cos, sine)


def place_body(counts_ref, shift_ref, box_ref, out_hbm, placed, sems):
    senders = box_ref.shape[0]
    per_tile = counts_ref.shape[0]
    tiles = shift_ref.shape[0] // per_tile
    me = lax.axis_index("dp")
    lane = lax.broadcasted_iota(jnp.int32, (TILE, TILE), 1)
    row = lax.broadcasted_iota(jnp.int32, (TILE, TILE), 0)
    inside = jnp.bitwise_and(lane, IMG_MAX - 1)
    image = lane // IMG_MAX
    copies = []
    for tile in range(tiles):
        goal = jnp.full((TILE, TILE), -1, jnp.int32)
        offset = jnp.int32(0)
        blocks = []
        for j in range(per_tile):
            count = counts_ref[j, me * tiles + tile]
            goal = jnp.where((image == j) & (inside < count), inside + offset, goal)
            offset = offset + count
            source = lax.rem(me + shift_ref[tile * per_tile + j], senders)
            blocks.append(box_ref[source])
        at = pl.ds(tile * TILE, TILE)
        placed[at, :] = jnp.dot(
            jnp.where(row == goal, 1.0, 0.0).astype(jnp.bfloat16),
            jnp.concatenate(blocks, axis=0),
            preferred_element_type=jnp.float32,
        ).astype(jnp.bfloat16)
        copy = pltpu.make_async_copy(placed.at[at], out_hbm.at[at], sems.at[tile])
        copy.start()
        copies.append(copy)
    for copy in copies:
        copy.wait()


def place_rows(counts, shift, box):
    senders, depth, columns = box.shape
    rows = shift.shape[0] * depth
    return pl.pallas_call(
        place_body,
        in_specs=[SCALARS] * 2 + [WHOLE],
        out_specs=FAR_MEMORY,
        out_shape=jax.ShapeDtypeStruct((rows, columns), jnp.bfloat16),
        scratch_shapes=[
            pltpu.VMEM((rows, columns), jnp.bfloat16),
            pltpu.SemaphoreType.DMA((rows // TILE,)),
        ],
        compiler_params=limit(8),
        name="place_rows",
    )(counts, shift, box)


def local(
    patches, ln_gain, ln_bias, w_proj, proj_bias, rms_gain, w_qkv, image_counts, source_shift
):
    senders = lax.axis_size("dp")
    counts = image_counts.T
    other = lax.ppermute(patches, "mp", SWAP)
    pin = lambda x: pltpu.with_memory_space_constraint(x, pltpu.HBM)
    own = norm_own(pin(patches), pin(ln_gain), pin(ln_bias))
    normed, plan = norm_other(counts, source_shift, own, other, ln_gain, ln_bias)
    near = project(plan, normed, w_proj, proj_bias, rms_gain)
    far = lax.ppermute(near, "mp", SWAP)
    part = first_half(plan, near, w_qkv)
    outbox = attend(plan, near, far, w_qkv, part, senders)
    in_box = lax.all_to_all(outbox, "dp", split_axis=0, concat_axis=0, tiled=True)
    return place_rows(counts, source_shift, in_box)


def solution(mesh):
    in_specs = (
        P(("dp", "mp"), None),
        P(),
        P(),
        P(None, "mp"),
        P("mp"),
        P(),
        P(None, "mp"),
        P(),
        P(),
    )
    out_specs = P("dp", "mp")
    return jax.shard_map(local, mesh=mesh, in_specs=in_specs, out_specs=out_specs, check_vma=False)
```

```python
import functools

import jax
import jax.numpy as jnp
import numpy as np
from jax import lax
from jax.experimental import pallas as pl
from jax.experimental.pallas import tpu as pltpu
from jax.sharding import PartitionSpec as P

HEAD_SIZE = 128
TILE = 128
QUERY_PER_KEY = 4
IMG_MAX = 16

norm_epsilon = 1e-05
rms_epsilon = 1e-05
rotary_base = 500000.0

SWAP = [(0, 1), (1, 0)]


WHOLE = pl.BlockSpec(memory_space=pltpu.VMEM)
SCALARS = pl.BlockSpec(memory_space=pltpu.SMEM)
FAR_MEMORY = pl.BlockSpec(memory_space=pltpu.HBM)
NORM_ROWS = 32
CUTS = (1024, 768, 256)
NARROW = 256
QKV_COLUMNS = 768
WINDOW = TILE + 2 * IMG_MAX
ROW_BOUNDS = (352, 384)


def limit(mib):
    return pltpu.CompilerParams(vmem_limit_bytes=mib * 1024 * 1024)


def rotary_tables(rows):
    half = HEAD_SIZE // 2
    frequency = rotary_base ** (-(np.arange(half, dtype=np.float64) * (2.0 / HEAD_SIZE)))
    angles = np.arange(rows, dtype=np.float64)[:, None] * frequency[None, :]
    cos = np.concatenate([np.cos(angles), np.cos(angles)], axis=-1)
    sine = np.concatenate([-np.sin(angles), np.sin(angles)], axis=-1)
    return jnp.asarray(cos.astype(np.float32)), jnp.asarray(sine.astype(np.float32))


def plan_body(counts_ref, shift_ref, after_ref, plan_ref):
    del after_ref
    images = shift_ref.shape[0]
    tile_images = counts_ref.shape[0]
    tiles = images // tile_images
    senders = counts_ref.shape[1] // tiles
    me = lax.axis_index("dp")
    shifts = [shift_ref[k] for k in range(images)]
    targets = [lax.rem(me - shift + senders, senders) for shift in shifts]
    places = [(k % tile_images, k // tile_images) for k in range(images)]
    sent = [counts_ref[row, to * tiles + at] for to, (row, at) in zip(targets, places)]
    mine = [counts_ref[row, me * tiles + at] for row, at in places]
    start = jnp.int32(0)
    for k in range(images):
        plan_ref[k] = start
        plan_ref[images + 1 + k] = targets[k]
        plan_ref[2 * images + 1 + k] = mine[k]
        plan_ref[3 * images + 1 + k] = lax.rem(me + shifts[k], senders)
        start = start + sent[k]
    plan_ref[images] = start


def make_plan(counts, shift, after):
    return pl.pallas_call(
        plan_body,
        in_specs=[SCALARS] * 2 + [pl.BlockSpec(memory_space=pl.ANY)],
        out_specs=SCALARS,
        out_shape=jax.ShapeDtypeStruct((4 * shift.shape[0] + 1,), jnp.int32),
        compiler_params=limit(1),
        cost_estimate=pl.CostEstimate(flops=10_000, bytes_accessed=10_000, transcendentals=0),
        name="make_plan",
    )(counts, shift, after)


def for_row_bound(total, most, run):
    below = jnp.int32(-1)
    for bound in (*ROW_BOUNDS, most):
        pl.when((total > below) & (total <= bound))(functools.partial(run, bound))
        below = jnp.int32(bound)


def normalised(rows, gain, bias):
    values = rows.astype(jnp.float32)
    width = values.shape[-1]
    row_mean = jnp.sum(values, axis=-1, keepdims=True) * (1.0 / width)
    centred = values - row_mean
    row_var = jnp.sum(centred * centred, axis=-1, keepdims=True) * (1.0 / width)
    scaled = centred * lax.rsqrt(row_var + norm_epsilon) * gain
    return (scaled + bias).astype(jnp.bfloat16)


def fill_normed(src_ref, gain_row, bias_row, dst_ref, first, count, base):
    def fill(i, carry):
        src = pl.multiple_of(first + i * NORM_ROWS, NORM_ROWS)
        dst = pl.multiple_of(base + first + i * NORM_ROWS, NORM_ROWS)
        dst_ref[pl.ds(dst, NORM_ROWS), :] = normalised(
            src_ref[pl.ds(src, NORM_ROWS), :], gain_row[...], bias_row[...]
        )
        return carry

    lax.fori_loop(0, count // NORM_ROWS, fill, 0, unroll=2)


NORM_PARTS = 4


def norm_own_body(rows_hbm, gain_hbm, bias_hbm, out_ref, rows_ref, gain_ref, bias_ref, gain_row, bias_row, sems):
    count, width = rows_ref.shape
    part = count // NORM_PARTS
    small = [
        pltpu.make_async_copy(gain_hbm, gain_ref, sems.at[NORM_PARTS]),
        pltpu.make_async_copy(bias_hbm, bias_ref, sems.at[NORM_PARTS + 1]),
    ]
    parts = [
        pltpu.make_async_copy(
            rows_hbm.at[pl.ds(n * part, part)], rows_ref.at[pl.ds(n * part, part)], sems.at[n]
        )
        for n in range(NORM_PARTS)
    ]
    for copy in small + parts:
        copy.start()
    for copy in small:
        copy.wait()
    gain_row[...] = gain_ref[...].reshape(1, width).astype(jnp.float32)
    bias_row[...] = bias_ref[...].reshape(1, width).astype(jnp.float32)
    for n in range(NORM_PARTS):
        parts[n].wait()
        fill_normed(rows_ref, gain_row, bias_row, out_ref, n * part, part, 0)


def norm_own(rows, gain, bias):
    count, width = rows.shape
    return pl.pallas_call(
        norm_own_body,
        in_specs=[FAR_MEMORY] * 3,
        out_specs=WHOLE,
        out_shape=jax.ShapeDtypeStruct((count, width), jnp.bfloat16),
        scratch_shapes=[
            pltpu.VMEM((count, width), jnp.bfloat16),
            pltpu.VMEM((width,), jnp.bfloat16),
            pltpu.VMEM((width,), jnp.bfloat16),
            pltpu.VMEM((1, width), jnp.float32),
            pltpu.VMEM((1, width), jnp.float32),
            pltpu.SemaphoreType.DMA((NORM_PARTS + 2,)),
        ],
        compiler_params=limit(8),
        cost_estimate=pl.CostEstimate(
            flops=8_000_000_000, bytes_accessed=4 * count * width, transcendentals=0
        ),
        name="norm_own",
    )(rows, gain, bias)


def norm_other_body(own_ref, other_ref, gain_ref, bias_ref, out_ref, gain_row, bias_row):
    half, width = own_ref.shape
    core = lax.axis_index("mp")
    out_ref[pl.ds(pl.multiple_of(core * half, half), half), :] = own_ref[...]
    gain_row[...] = gain_ref[...].reshape(1, width).astype(jnp.float32)
    bias_row[...] = bias_ref[...].reshape(1, width).astype(jnp.float32)
    fill_normed(
        other_ref, gain_row, bias_row, out_ref, 0, half, pl.multiple_of((1 - core) * half, half)
    )


def norm_other(own, other, gain, bias):
    half, width = own.shape
    return pl.pallas_call(
        norm_other_body,
        in_specs=[WHOLE] * 4,
        out_specs=WHOLE,
        out_shape=jax.ShapeDtypeStruct((2 * half, width), jnp.bfloat16),
        scratch_shapes=[pltpu.VMEM((1, width), jnp.float32)] * 2,
        compiler_params=limit(6),
        cost_estimate=pl.CostEstimate(
            flops=10 * half * width, bytes_accessed=4 * half * width, transcendentals=0
        ),
        name="norm_other",
    )(own, other, gain, bias)


def project_body(
    plan_ref, normed_ref, w_ref, add_ref, rms_ref,
    out_ref, add_row, rms_row, squares, acc_even, acc_odd,
):
    rows = normed_ref.shape[0]
    columns = w_ref.shape[1]
    total = plan_ref[plan_ref.shape[0] // 4]
    mine = pl.multiple_of(lax.axis_index("mp") * columns, columns)
    add_row[...] = add_ref[...].reshape(1, columns).astype(jnp.float32)
    rms_row[...] = rms_ref[...].reshape(1, 2 * columns).astype(jnp.float32)

    def run(bound):
        used = pl.ds(0, bound)

        def product(first, width, acc):
            acc[used, 0:width] = jnp.dot(
                normed_ref[used, :], w_ref[:, pl.ds(first, width)],
                preferred_element_type=jnp.float32,
            )

        def post(first, width, acc):
            pre = acc[used, 0:width] + add_row[:, pl.ds(first, width)]
            value = pre * (1.0 + lax.erf(pre * np.float32(0.5**0.5))) * 0.5
            value = value.astype(jnp.bfloat16).astype(jnp.float32)
            gain = rms_row[:, pl.ds(pl.multiple_of(mine + first, NARROW), width)]
            out_ref[used, pl.ds(first, width)] = (value * gain).astype(jnp.bfloat16)
            square = sum(
                value[:, c : c + 128] * value[:, c : c + 128] for c in range(0, width, 128)
            )
            squares[used, :] = squares[used, :] + square

        squares[...] = jnp.zeros_like(squares)
        if bound < rows:
            first, waiting = 0, None
            for n, width in enumerate(CUTS):
                acc = (acc_even, acc_odd)[n % 2]
                product(first, width, acc)
                if waiting is not None:
                    post(*waiting)
                waiting = (first, width, acc)
                first += width
            post(*waiting)
        else:

            def block(n, carry):
                at = pl.multiple_of(n * NARROW, NARROW)
                product(at, NARROW, acc_even)
                post(at, NARROW, acc_even)
                return carry

            lax.fori_loop(0, columns // NARROW, block, 0)
        row_sum = jnp.sum(squares[used, :], axis=-1, keepdims=True)
        high = row_sum.astype(jnp.bfloat16).astype(jnp.float32)
        lane = lax.broadcasted_iota(jnp.int32, (bound, 128), 1)
        out_ref[used, columns : columns + 128] = jnp.where(
            lane < 64, high, row_sum - high
        ).astype(jnp.bfloat16)

    for_row_bound(total, rows, run)


def project(plan, normed, w_proj, proj_bias, rms_gain):
    rows, width = normed.shape
    columns = w_proj.shape[1]
    return pl.pallas_call(
        project_body,
        in_specs=[SCALARS] + [WHOLE] * 4,
        out_specs=WHOLE,
        scratch_shapes=[
            pltpu.VMEM((1, columns), jnp.float32),
            pltpu.VMEM((1, 2 * columns), jnp.float32),
            pltpu.VMEM((rows, 128), jnp.float32),
            pltpu.VMEM((rows, CUTS[0]), jnp.float32),
            pltpu.VMEM((rows, CUTS[1]), jnp.float32),
        ],
        out_shape=jax.ShapeDtypeStruct((rows, columns + 128), jnp.bfloat16),
        compiler_params=limit(18),
        cost_estimate=pl.CostEstimate(
            flops=2 * rows * width * columns,
            bytes_accessed=2 * width * columns,
            transcendentals=rows * columns,
        ),
        name="project",
    )(plan, normed, w_proj, proj_bias, rms_gain)


def first_half_body(plan_ref, gained_ref, w_ref, part_ref):
    rows = gained_ref.shape[0]
    depth = w_ref.shape[0] // 2
    mine = pl.multiple_of(lax.axis_index("mp") * depth, depth)
    total = plan_ref[plan_ref.shape[0] // 4]

    def run(bound):
        def block(j, carry):
            at = pl.multiple_of(j * QKV_COLUMNS, QKV_COLUMNS)
            part_ref[pl.ds(0, bound), pl.ds(at, QKV_COLUMNS)] = jnp.dot(
                gained_ref[pl.ds(0, bound), pl.ds(0, depth)],
                w_ref[pl.ds(mine, depth), pl.ds(at, QKV_COLUMNS)],
                preferred_element_type=jnp.float32,
            )
            return carry

        lax.fori_loop(0, w_ref.shape[1] // QKV_COLUMNS, block, 0)

    for_row_bound(total, rows, run)


def first_half(plan, gained, w_qkv):
    rows = gained.shape[0]
    depth, columns = w_qkv.shape
    return pl.pallas_call(
        first_half_body,
        in_specs=[SCALARS] + [WHOLE] * 2,
        out_specs=WHOLE,
        out_shape=jax.ShapeDtypeStruct((rows, columns), jnp.float32),
        compiler_params=limit(6),
        cost_estimate=pl.CostEstimate(
            flops=rows * depth * columns,
            bytes_accessed=depth * columns + 4 * rows * columns,
            transcendentals=0,
        ),
        name="first_half",
    )(plan, gained, w_qkv)


def attend_body(
    plan_ref, near_ref, far_ref, w_ref, part_ref, cos_ref, sine_ref,
    out_ref, factor, ones, align, heads, turned_rows, queries, keys, values, scores,
):
    groups, padded, width = turned_rows.shape
    rows = far_ref.shape[0]
    depth = w_ref.shape[0] // 2
    images = plan_ref.shape[0] // 4
    per_tile = TILE // IMG_MAX
    tiles = rows // TILE
    pair = 2 * HEAD_SIZE
    far = pl.multiple_of((1 - lax.axis_index("mp")) * depth, depth)
    starts = [plan_ref[k] for k in range(images)]
    total = plan_ref[images]
    targets = [plan_ref[images + 1 + k] for k in range(images)]
    bases = [
        pl.multiple_of((starts[tile * per_tile] // IMG_MAX) * IMG_MAX, IMG_MAX)
        for tile in range(tiles)
    ]

    def prepare():
        column = lax.broadcasted_iota(jnp.int32, (IMG_MAX, WINDOW), 1)
        distance = column - lax.broadcasted_iota(jnp.int32, (IMG_MAX, WINDOW), 0)
        empty = jnp.zeros((groups, tiles, HEAD_SIZE, HEAD_SIZE), jnp.bfloat16)
        for tile in range(tiles):
            for j in range(per_tile):
                align[tile, j * IMG_MAX : (j + 1) * IMG_MAX, :] = jnp.where(
                    distance == starts[tile * per_tile + j] - bases[tile], 1.0, 0.0
                ).astype(jnp.bfloat16)
        for kept in (keys, values):
            kept[:, :, 0:HEAD_SIZE, HEAD_SIZE:pair] = empty
            kept[:, :, HEAD_SIZE:pair, 0:HEAD_SIZE] = empty
        side = lax.broadcasted_iota(jnp.int32, (pair, pair), 0) // HEAD_SIZE
        ones[...] = jnp.where(
            side == lax.broadcasted_iota(jnp.int32, (pair, pair), 1) // HEAD_SIZE, 1.0, 0.0
        ).astype(jnp.bfloat16)

    q_at = jnp.bitwise_and(lax.broadcasted_iota(jnp.int32, (pair, pair), 0), TILE - 1)
    k_at = jnp.bitwise_and(lax.broadcasted_iota(jnp.int32, (pair, pair), 1), TILE - 1)
    allowed = (q_at >= k_at) & ((q_at // IMG_MAX) == (k_at // IMG_MAX))

    def line_up(group):
        for tile in range(tiles):
            window = turned_rows[group, pl.ds(bases[tile], WINDOW), :]
            placed = jnp.dot(align[tile], window, preferred_element_type=jnp.float32).astype(
                jnp.bfloat16
            )
            queries[group, tile * TILE : (tile + 1) * TILE, :] = placed[:, 0 : 2 * pair]
            for kept, n in ((keys, QUERY_PER_KEY), (values, QUERY_PER_KEY + 1)):
                block = placed[:, n * HEAD_SIZE : (n + 1) * HEAD_SIZE]
                kept[group, tile, 0:TILE, 0:HEAD_SIZE] = block
                kept[group, tile, TILE : 2 * TILE, HEAD_SIZE:pair] = block

    def score(group):
        for tile in range(tiles):
            at = slice(tile * TILE, (tile + 1) * TILE)
            stacked = jnp.concatenate(
                [queries[group, at, 0:pair], queries[group, at, pair : 2 * pair]], axis=0
            )
            scores[group, tile] = lax.dot_general(
                stacked, keys[group, tile], (((1,), (1,)), ((), ())),
                preferred_element_type=jnp.float32,
            )

    def weigh(group):
        for tile in range(tiles):
            seen = jnp.where(allowed, scores[group, tile] * np.float32(HEAD_SIZE**-0.5), -1e30)
            weights = jnp.concatenate(
                [
                    jnp.exp(half - jnp.max(half, axis=-1, keepdims=True)).astype(jnp.bfloat16)
                    for half in (seen[:, 0:HEAD_SIZE], seen[:, HEAD_SIZE:pair])
                ],
                axis=1,
            )
            weighed = jnp.dot(weights, values[group, tile], preferred_element_type=jnp.float32)
            row_sum = jnp.dot(weights, ones[...], preferred_element_type=jnp.float32)
            attended = (weighed * (1.0 / row_sum)).astype(jnp.bfloat16)
            for j in range(per_tile):
                target = targets[tile * per_tile + j]
                for n in range(2):
                    column = group * QUERY_PER_KEY * HEAD_SIZE + n * pair
                    out_ref[target, :, column : column + pair] = attended[
                        n * TILE + j * IMG_MAX : n * TILE + (j + 1) * IMG_MAX, :
                    ]

    def run(bound):
        used = slice(0, bound)
        both = near_ref[used, depth:].astype(jnp.float32) + far_ref[used, depth:].astype(
            jnp.float32
        )
        squares = both[:, 0:1] + both[:, 64:65]
        factor[used, :] = jnp.broadcast_to(
            lax.rsqrt(squares * (1.0 / (2 * depth)) + rms_epsilon), (bound, HEAD_SIZE)
        )

        def piece(group, first, size):
            at = pl.ds(group * width + first, size)
            heads[group, used, pl.ds(first, size)] = part_ref[used, at] + jnp.dot(
                far_ref[used, 0:depth], w_ref[pl.ds(far, depth), at],
                preferred_element_type=jnp.float32,
            )

        def product(group, first, last):
            if bound < rows:
                piece(group, first, last - first)
            else:

                def narrow(n, carry):
                    piece(group, pl.multiple_of(first + n * NARROW, NARROW), NARROW)
                    return carry

                lax.fori_loop(0, (last - first) // NARROW, narrow, 0)

        def rotate(group):
            for n in range(QUERY_PER_KEY + 2):
                at = slice(n * HEAD_SIZE, (n + 1) * HEAD_SIZE)
                rows_in = heads[group, used, at] * factor[used, :]
                if n <= QUERY_PER_KEY:
                    turned = pltpu.roll(rows_in, HEAD_SIZE // 2, 1)
                    rows_in = rows_in * cos_ref[used, :] + turned * sine_ref[used, :]
                turned_rows[group, used, at] = rows_in.astype(jnp.bfloat16)

        product(0, 0, width)
        prepare()
        turned_rows[:, bound:, :] = jnp.zeros((groups, padded - bound, width), jnp.bfloat16)
        for group in range(1, groups):
            product(group, 0, width)
            rotate(group - 1)
            line_up(group - 1)
            score(group - 1)
        rotate(groups - 1)
        line_up(groups - 1)
        score(groups - 1)
        for group in range(groups):
            weigh(group)

    for_row_bound(total, rows, run)


def attend(plan, near, far, w_qkv, part, senders):
    rows = far.shape[0]
    block = (QUERY_PER_KEY + 2) * HEAD_SIZE
    depth, columns = w_qkv.shape
    groups = columns // block
    out_columns = groups * QUERY_PER_KEY * HEAD_SIZE
    padded = rows + WINDOW
    pair = 2 * HEAD_SIZE
    tiles = rows // TILE
    cos, sine = rotary_tables(rows)
    return pl.pallas_call(
        attend_body,
        in_specs=[SCALARS] + [WHOLE] * 6,
        out_specs=WHOLE,
        scratch_shapes=[
            pltpu.VMEM((rows, HEAD_SIZE), jnp.float32),
            pltpu.VMEM((pair, pair), jnp.bfloat16),
            pltpu.VMEM((tiles, TILE, WINDOW), jnp.bfloat16),
            pltpu.VMEM((groups, rows, block), jnp.float32),
            pltpu.VMEM((groups, padded, block), jnp.bfloat16),
            pltpu.VMEM((groups, rows, 2 * pair), jnp.bfloat16),
            pltpu.VMEM((groups, tiles, pair, pair), jnp.bfloat16),
            pltpu.VMEM((groups, tiles, pair, pair), jnp.bfloat16),
            pltpu.VMEM((groups, tiles, pair, pair), jnp.float32),
        ],
        out_shape=jax.ShapeDtypeStruct((senders, IMG_MAX, out_columns), jnp.bfloat16),
        compiler_params=limit(20),
        cost_estimate=pl.CostEstimate(
            flops=rows * depth * columns, bytes_accessed=depth * columns, transcendentals=0
        ),
        name="attend",
    )(plan, near, far, w_qkv, part, cos, sine)


def place_body(plan_ref, box_ref, out_hbm, placed, sems):
    images = plan_ref.shape[0] // 4
    per_tile = TILE // IMG_MAX
    tiles = images // per_tile
    lane = lax.broadcasted_iota(jnp.int32, (TILE, TILE), 1)
    row = lax.broadcasted_iota(jnp.int32, (TILE, TILE), 0)
    inside = jnp.bitwise_and(lane, IMG_MAX - 1)
    image = lane // IMG_MAX
    copies = []
    for tile in range(tiles):
        goal = jnp.full((TILE, TILE), -1, jnp.int32)
        offset = jnp.int32(0)
        blocks = []
        for j in range(per_tile):
            count = plan_ref[2 * images + 1 + tile * per_tile + j]
            goal = jnp.where((image == j) & (inside < count), inside + offset, goal)
            offset = offset + count
            blocks.append(box_ref[plan_ref[3 * images + 1 + tile * per_tile + j]])
        at = pl.ds(tile * TILE, TILE)
        placed[at, :] = jnp.dot(
            jnp.where(row == goal, 1.0, 0.0).astype(jnp.bfloat16),
            jnp.concatenate(blocks, axis=0),
            preferred_element_type=jnp.float32,
        ).astype(jnp.bfloat16)
        copy = pltpu.make_async_copy(placed.at[at], out_hbm.at[at], sems.at[tile])
        copy.start()
        copies.append(copy)
    for copy in copies:
        copy.wait()


def place_rows(plan, box):
    depth, columns = box.shape[1:]
    rows = plan.shape[0] // 4 * depth
    return pl.pallas_call(
        place_body,
        in_specs=[SCALARS, WHOLE],
        out_specs=FAR_MEMORY,
        out_shape=jax.ShapeDtypeStruct((rows, columns), jnp.bfloat16),
        scratch_shapes=[
            pltpu.VMEM((rows, columns), jnp.bfloat16),
            pltpu.SemaphoreType.DMA((rows // TILE,)),
        ],
        compiler_params=limit(8),
        name="place_rows",
    )(plan, box)


def local(
    patches, ln_gain, ln_bias, w_proj, proj_bias, rms_gain, w_qkv, image_counts, source_shift
):
    senders = lax.axis_size("dp")
    counts = image_counts.T
    other = lax.ppermute(patches, "mp", SWAP)
    pin = lambda x: pltpu.with_memory_space_constraint(x, pltpu.HBM)
    own = norm_own(pin(patches), pin(ln_gain), pin(ln_bias))
    plan = make_plan(counts, source_shift, own)
    normed = norm_other(own, other, ln_gain, ln_bias)
    near = project(plan, normed, w_proj, proj_bias, rms_gain)
    far = lax.ppermute(near, "mp", SWAP)
    part = first_half(plan, near, w_qkv)
    outbox = attend(plan, near, far, w_qkv, part, senders)
    in_box = lax.all_to_all(outbox, "dp", split_axis=0, concat_axis=0, tiled=True)
    return place_rows(plan, in_box)


def solution(mesh):
    in_specs = (
        P(("dp", "mp"), None),
        P(),
        P(),
        P(None, "mp"),
        P("mp"),
        P(),
        P(None, "mp"),
        P(),
        P(),
    )
    out_specs = P("dp", "mp")
    return jax.shard_map(local, mesh=mesh, in_specs=in_specs, out_specs=out_specs, check_vma=False)
```
